32 devices in a mesh: dp: 8 (over z, core), tensor: 4 (over y, x).
Axes of the slice: x: 2, y: 2, z: 4, core: 2. Of those that a mesh axis runs over, the one named last changes fastest.
Arguments:
- tokens: bfloat16 [4096, 2048], P('dp'), may hold values from -6 to 6
- segments: int32 [8, 512], P('dp'), may hold values from 0 to 1, never falling along the last dimension, each value on 1 to 511 neighbouring positions
- expert_ids: int32 [4096, 6], P('dp'), may hold values from 0 to 31, all different within a row; in each aligned block of 512 rows (0 to 511, 512 to 1023, ...) at most 144 rows name the same one
- route_weight: float32 [4096, 6], P('dp'), may hold values from 0.1 to 1
- norm1_gain: bfloat16 [2048], P(('dp', 'tensor')), may hold values from 0.5 to 1.5
- q_weight: bfloat16 [2048, 3072], P('dp', 'tensor'), may hold values from -0.125 to 0.125
- kva_weight: bfloat16 [2048, 576], P(('dp', 'tensor')), may hold values from -0.125 to 0.125
- kv_gain: bfloat16 [512], P(('dp', 'tensor')), may hold values from 0.5 to 1.5
- kvb_weight: bfloat16 [512, 4096], P('dp', 'tensor'), may hold values from -0.25 to 0.25
- out_weight: bfloat16 [2048, 2048], P('tensor', 'dp'), may hold values from -1 to 1
- norm2_gain: bfloat16 [2048], P(('dp', 'tensor')), may hold values from 0.5 to 1.5
- shared_gate: bfloat16 [2048, 2816], P('dp', 'tensor'), may hold values from -0.125 to 0.125
- shared_up: bfloat16 [2048, 2816], P('dp', 'tensor'), may hold values from -0.125 to 0.125
- shared_down: bfloat16 [2816, 2048], P('tensor', 'dp'), may hold values from -0.21875 to 0.21875
- expert_gate: bfloat16 [32, 2048, 1408], P('dp', None, 'tensor'), may hold values from -0.125 to 0.125
- expert_up_projection: bfloat16 [32, 2048, 1408], P('dp', None, 'tensor'), may hold values from -0.125 to 0.125
- expert_down: bfloat16 [32, 1408, 2048], P('dp', 'tensor'), may hold values from -0.3125 to 0.3125
- cotangent: bfloat16 [4096, 2048], P('dp'), may hold values from -6 to 6
Outputs:
- output: bfloat16 [4096, 2048], P('dp')
- grad_tokens: float32 [4096, 2048], P('dp')
- grad_norm1_gain: float32 [2048], P(('dp', 'tensor'))
- grad_q_weight: float32 [2048, 3072], P('dp', 'tensor')
- grad_kva_weight: float32 [2048, 576], P(('dp', 'tensor'))
- grad_kv_gain: float32 [512], P(('dp', 'tensor'))
- grad_kvb_weight: float32 [512, 4096], P('dp', 'tensor')
- grad_out_weight: float32 [2048, 2048], P('tensor', 'dp')
- grad_norm2_gain: float32 [2048], P(('dp', 'tensor'))
- grad_shared_gate: float32 [2048, 2816], P('dp', 'tensor')
- grad_shared_up: float32 [2048, 2816], P('dp', 'tensor')
- grad_shared_down: float32 [2816, 2048], P('tensor', 'dp')
- grad_expert_gate: float32 [32, 2048, 1408], P('dp', None, 'tensor')
- grad_expert_up: float32 [32, 2048, 1408], P('dp', None, 'tensor')
- grad_expert_down: float32 [32, 1408, 2048], P('dp', 'tensor')
The draws below stay inside these ranges and needn't reach their ends.
Inputs may be any that keep to these rules, and one draw needn't show every extreme that they name: `segments`: each row holds 2 sequences laid end to end; numbers never fall along a row; each sequence has 1 to 511 tokens. `expert_ids`: each token names 6 different experts; among the 512 tokens of one index of dp no expert is named more than 144 times, a bound that some block reaches.
All inputs are finite; a program needn't handle non-finite values.
Results may differ from the reference program's by a relative error of at most 0.025.
Values may be sent and summed in bfloat16 or wider, within the bound.
A program may use at most 384 MiB of HBM per device.

```python
import math
import jax
import jax.numpy as jnp
import numpy as np
from jax import lax

D = 2048
H = 16
NOPE = 128
ROPE = 64
VDIM = 128
LATENT = 512
FF_E = 1408
SFF = 2816
TOPK = 6
EXPERTS = 32
TOK_DEV = 512
TOKENS = 4096
SEGS = 2
SEQ_MOST = 511
CAP = 144
N_DP = 8
N_TENSOR = 4


def steps_of(rng, dims, pieces, low, top_value):
    gain = 1.0
    for position, shards_of in pieces:
        heights = jax.random.uniform(jax.random.fold_in(jax.random.fold_in(rng, 6), position), (shards_of,), jnp.float32, low / len(pieces), top_value / len(pieces))
        gain = gain * jnp.repeat(jnp.exp(heights), dims[position] // shards_of).reshape((-1,) + (1,) * (len(dims) - 1 - position))
    return gain


def split_up(number_of, total, bound, skew):
    loads = [(1 << 20) // math.isqrt(grade ** skew) + 1 for grade in range(2, number_of + 1)]
    spare, counts = total - bound - (number_of - 1), [1] * (number_of - 1)
    while spare > 0:
        candidates = [i for i in range(number_of - 1) if counts[i] < bound]
        mass, left = sum([loads[i] for i in candidates]), spare
        for i in candidates:
            extra = min(bound - counts[i], max(1, left * loads[i] // mass), spare)
            counts[i] = counts[i] + extra
            spare = spare - extra
    return np.array([bound] + counts)


def ragged_sizes(own_key, number_of, total, reach, slope):
    if number_of == 2:
        one = jax.random.randint(own_key, (), max(1, total - reach), min(reach, total - 1) + 1)
        return jnp.stack([one, total - one])
    sizes = jnp.asarray(split_up(number_of, total, reach, slope), jnp.int32)
    couples = (number_of - 1) // 2
    donor, receiver = sizes[1:1 + 2 * couples:2], sizes[2:2 + 2 * couples:2]
    room = jnp.minimum(donor - 1, reach - receiver)
    moved = jax.random.randint(jax.random.fold_in(own_key, 1), (couples,), 0, 1 << 20) % (room + 1)
    sizes = sizes.at[1:1 + 2 * couples:2].set(donor - moved).at[2:2 + 2 * couples:2].set(receiver + moved)
    return sizes[jax.random.permutation(jax.random.fold_in(own_key, 2), number_of)]


def deal_out(rng, own, number, rows, number_of, top, bound, skew):
    order = jax.random.permutation(rng, number_of)
    crowded, common = shares(number_of, rows * top, bound, skew, True), shares(number_of, rows * top, bound, skew, False)
    places = jnp.arange(number_of)

    def named(tallies, rotation):
        used = int((tallies > 0).sum())
        fixed = max(1, used // 4)
        moved = fixed + (places - fixed + rotation * (used - fixed)) % max(1, number_of - fixed)
        return jnp.zeros((number_of,), jnp.int32).at[order[jnp.where(places < fixed, places, moved)]].set(jnp.asarray(tallies, jnp.int32))

    tallies = jnp.where(number % 4 == 0, named(crowded, number // 4), named(common, number - number // 4 - 1))
    mixed = jax.random.permutation(jax.random.fold_in(own, 3), number_of)
    donor, taker = mixed[0:number_of // 2 * 2:2], mixed[1:number_of // 2 * 2:2]
    margin = jnp.minimum(tallies[donor] - 1, bound - tallies[taker]) // 2
    margin = jnp.where((donor == order[0]) | (taker == order[0]) | (tallies[taker] == 0), 0, jnp.maximum(margin, 0))
    moved = jax.random.randint(jax.random.fold_in(own, 4), (number_of // 2,), 0, 1 << 20) % (margin + 1)
    tallies = tallies.at[donor].add(-moved).at[taker].add(moved)
    items = jnp.searchsorted(jnp.cumsum(tallies), jnp.arange(rows * top), side="right").astype(jnp.int32)
    table = items.reshape(top, rows).T
    table = table[jax.random.permutation(jax.random.fold_in(own, 1), rows)]
    rotation = jax.random.randint(jax.random.fold_in(own, 2), (rows, 1), 0, top)
    return jnp.take_along_axis(table, (jnp.arange(top)[None, :] + rotation) % top, axis=1)


def shares(amount, total, reach, lean, full):
    portions = [(1 << 20) // math.isqrt(grade ** lean) + 1 for grade in range(1, amount + 1)]
    largest = reach if full else min(reach, max(-(-total // amount), total * portions[0] // sum(portions)))
    least = 1 if total - largest >= amount - 1 else 0
    given, surplus = [largest] + [least] * (amount - 1), total - largest - least * (amount - 1)
    while surplus > 0:
        movable = [i for i in range(1, amount) if given[i] < largest] or [i for i in range(1, amount) if given[i] < reach]
        mass, budget = sum([portions[i] for i in movable]), surplus
        for i in movable:
            extra = min(reach - given[i], max(1, budget * portions[i] // mass), surplus)
            given[i] = given[i] + extra
            surplus = surplus - extra
    return np.array(given)


def normal_values(rng, extent, width, most, pieces=(), kind=jnp.bfloat16):
    loudness = steps_of(rng, extent, pieces, -0.22, 0.18) if pieces else 1.0
    entries = jax.random.normal(rng, extent, jnp.float32) * width * loudness
    return jnp.minimum(jnp.maximum(entries, -most), most).astype(kind)


def setup_inputs(seed: int = 0) -> dict:
    keys = jax.random.split(jax.random.key(seed), 19)
    tokens = normal_values(keys[0], (TOKENS, D), 1.0, 6.0, ((0, 8),))
    segments = jax.vmap(lambda own: jnp.searchsorted(jnp.cumsum(ragged_sizes(own, SEGS, TOK_DEV, SEQ_MOST, 2)), jnp.arange(TOK_DEV), side="right"))(jax.random.split(keys[1], N_DP)).reshape((N_DP, TOK_DEV)).astype(jnp.int32)
    expert_ids_keys = jax.random.split(jax.random.fold_in(keys[2], 1), TOKENS // TOK_DEV)
    expert_ids_turns = jax.random.permutation(jax.random.fold_in(keys[2], 3), TOKENS // TOK_DEV)
    expert_ids = jax.vmap(lambda own, number: deal_out(jax.random.fold_in(keys[2], 2), own, number, TOK_DEV, EXPERTS, TOPK, CAP, 2))(expert_ids_keys, expert_ids_turns).reshape((TOKENS, TOPK))
    route_weight = jnp.clip(jnp.exp(math.log(1.0) - 2.3025851 * jax.random.uniform(keys[3], (TOKENS, TOPK), jnp.float32) ** steps_of(keys[3], (TOKENS, TOPK), ((0, 8),), -0.2, 0.2)), 0.1, 1.0)
    norm1_gain = jnp.clip(1.0 + 0.1 * jax.random.normal(keys[4], (D,), jnp.float32), 0.5, 1.5).astype(jnp.bfloat16)
    q_weight = normal_values(keys[5], (D, H * (NOPE + ROPE)), D ** -0.5, 0.125, ((0, 8), (1, 4)))
    kva_weight = normal_values(keys[6], (D, LATENT + ROPE), D ** -0.5, 0.125, ((0, 32),))
    kv_gain = jnp.clip(1.0 + 0.1 * jax.random.normal(keys[7], (LATENT,), jnp.float32), 0.5, 1.5).astype(jnp.bfloat16)
    kvb_weight = normal_values(keys[8], (LATENT, H * (NOPE + VDIM)), LATENT ** -0.5, 0.25, ((0, 8), (1, 4)))
    out_weight = normal_values(keys[9], (H * VDIM, D), (H * VDIM // 64) ** -0.5, 1.0, ((0, 4), (1, 8)))
    norm2_gain = jnp.clip(1.0 + 0.1 * jax.random.normal(keys[10], (D,), jnp.float32), 0.5, 1.5).astype(jnp.bfloat16)
    shared_gate = normal_values(keys[11], (D, SFF), D ** -0.5, 0.125, ((0, 8), (1, 4)))
    shared_up = normal_values(keys[12], (D, SFF), D ** -0.5, 0.125, ((0, 8), (1, 4)))
    shared_down = normal_values(keys[13], (SFF, D), (SFF // 4) ** -0.5, 0.21875, ((0, 4), (1, 8)))
    expert_gate = normal_values(keys[14], (EXPERTS, D, FF_E), D ** -0.5, 0.125, ((0, 8), (2, 4)))
    expert_up_projection = normal_values(keys[15], (EXPERTS, D, FF_E), D ** -0.5, 0.125, ((0, 8), (2, 4)))
    expert_down = normal_values(keys[16], (EXPERTS, FF_E, D), (FF_E // 4) ** -0.5, 0.3125, ((0, 8), (1, 4)))
    cotangent = normal_values(keys[17], (TOKENS, D), 1.0, 6.0, ((0, 8),))
    return {"tokens": tokens, "segments": segments, "expert_ids": expert_ids, "route_weight": route_weight, "norm1_gain": norm1_gain, "q_weight": q_weight, "kva_weight": kva_weight, "kv_gain": kv_gain, "kvb_weight": kvb_weight, "out_weight": out_weight, "norm2_gain": norm2_gain, "shared_gate": shared_gate, "shared_up": shared_up, "shared_down": shared_down, "expert_gate": expert_gate, "expert_up_projection": expert_up_projection, "expert_down": expert_down, "cotangent": cotangent}


epsilon = 1e-06
theta_base = 10000.0
highest = lax.Precision.HIGHEST

@jax.custom_vjp
def low(v):
    return lax.optimization_barrier(v.astype(jnp.bfloat16)).astype(jnp.float32)

@jax.custom_vjp
def low_back(v):
    return v

def low_keep(v):
    return (low(v), None)

def low_pass(kept, grad):
    return (grad,)

def back_keep(v):
    return (v, None)

def back_low(kept, grad):
    return (low(grad),)
low.defvjp(low_keep, low_pass)
low_back.defvjp(back_keep, back_low)

def normalize(vector):
    return vector * lax.rsqrt(lax.optimization_barrier(jnp.mean(vector * vector, axis=-1, keepdims=True)) + epsilon)

def rotate(vector, cosine, sine_part):
    half_width = vector.shape[-1] // 2
    lower_half = vector[..., :half_width]
    upper_half = vector[..., half_width:]
    return jnp.concatenate([lower_half * cosine - upper_half * sine_part, upper_half * cosine + lower_half * sine_part], axis=-1)

def angles(segment_row):
    seq_len = segment_row.shape[0]
    member = segment_row[:, None] == jnp.arange(SEGS, dtype=jnp.int32)[None, :]
    seq_sizes = lax.optimization_barrier(jnp.sum(member.astype(jnp.int32), axis=0))
    starts = jnp.cumsum(seq_sizes) - seq_sizes
    seq_first = lax.optimization_barrier(jnp.sum(jnp.where(member, starts[None, :], 0), axis=1))
    seq_place = (jnp.arange(seq_len, dtype=jnp.int32) - seq_first).astype(jnp.float32)
    inv_freq = theta_base ** (-2.0 * jnp.arange(ROPE // 2, dtype=jnp.float32) / ROPE)
    angle_all = seq_place[:, None] * inv_freq[None, :]
    return (jnp.cos(angle_all), jnp.sin(angle_all))

def attend(normed, segment_row, q_weight, kva_weight, kv_gain, kvb_weight):
    seq_len = normed.shape[0]
    group_heads = H // N_TENSOR
    score_scale = (NOPE + ROPE) ** (-0.5)
    cosine, sine_part = angles(segment_row)
    queries = low_back(jnp.dot(normed, q_weight, precision=highest)).reshape(seq_len, H, NOPE + ROPE)
    q_rot = low(jnp.concatenate([queries[..., :NOPE], rotate(queries[..., NOPE:], cosine[:, None, :], sine_part[:, None, :])], axis=-1))
    compressed = jnp.dot(normed, kva_weight, precision=highest)
    copies = low_back(jnp.broadcast_to(compressed[None], (N_TENSOR, seq_len, LATENT + ROPE)))
    latent = low(normalize(copies[..., :LATENT]) * kv_gain)
    key_rot = low(rotate(copies[..., LATENT:], cosine, sine_part))
    weight_groups = kvb_weight.reshape(LATENT, N_TENSOR, group_heads * (NOPE + VDIM))
    keyval = low(low_back(jnp.einsum('gtl,lgf->gtf', latent, weight_groups, precision=highest)))
    keyval = keyval.reshape(N_TENSOR, seq_len, group_heads, NOPE + VDIM)
    q_groups = q_rot.reshape(seq_len, N_TENSOR, group_heads, NOPE + ROPE)
    scores = jnp.einsum('tghd,gshd->ghts', q_groups[..., :NOPE], keyval[..., :NOPE], precision=highest)
    scores = scores + jnp.einsum('tghr,gsr->ghts', q_groups[..., NOPE:], key_rot, precision=highest)
    scores = low_back(scores * score_scale)
    positions = jnp.arange(seq_len, dtype=jnp.int32)
    allowed = (segment_row[:, None] == segment_row[None, :]) & (positions[None, :] <= positions[:, None])
    scores = jnp.where(allowed[None, None], scores, -1000000000.0)
    attn_probs = jax.nn.softmax(scores, axis=-1)
    mixed_heads = low(low_back(jnp.einsum('ghts,gshv->tghv', low(attn_probs), keyval[..., NOPE:], precision=highest)))
    return mixed_heads.reshape(seq_len, H * VDIM)

def experts_one(feedforward_normed_input, row_token_index, row_gate_weights, row_valid_mask, gate_w, up_w, down_w):
    slice_width = FF_E // N_TENSOR
    inputs = feedforward_normed_input[row_token_index] * row_valid_mask[:, None]
    copies = low_back(jnp.broadcast_to(inputs[None], (N_TENSOR,) + inputs.shape))
    gate_act = low_back(jnp.einsum('grd,dgf->grf', copies, gate_w.reshape(D, N_TENSOR, slice_width), precision=highest))
    up_act = low_back(jnp.einsum('grd,dgf->grf', copies, up_w.reshape(D, N_TENSOR, slice_width), precision=highest))
    hidden = low(jax.nn.silu(gate_act) * up_act)
    slice_out = low(low_back(jnp.einsum('grf,gfd->grd', hidden, down_w.reshape(N_TENSOR, slice_width, D), precision=highest)))
    return lax.optimization_barrier(jnp.sum(slice_out, axis=0)) * row_gate_weights[:, None]

def slot_tables(expert_ids, route_weight):
    flat_ids = expert_ids.reshape(N_DP, TOK_DEV * TOPK)
    member = (flat_ids[:, :, None] == jnp.arange(EXPERTS, dtype=jnp.int32)[None, None, :]).astype(jnp.int32)
    slot_rank = lax.optimization_barrier(jnp.sum((jnp.cumsum(member, axis=1) - member) * member, axis=2))
    source = jnp.arange(N_DP, dtype=jnp.int32)[:, None]
    column = (source * CAP + slot_rank).reshape(-1)
    token_row = (source * TOK_DEV + jnp.arange(TOK_DEV * TOPK, dtype=jnp.int32)[None, :] // TOPK).reshape(-1)
    expert_row = flat_ids.reshape(-1)
    row_token_index = jnp.zeros((EXPERTS, N_DP * CAP), jnp.int32).at[expert_row, column].set(token_row)
    row_gate_weights = jnp.zeros((EXPERTS, N_DP * CAP), jnp.float32).at[expert_row, column].set(route_weight.reshape(-1))
    row_valid_mask = jnp.zeros((EXPERTS, N_DP * CAP), jnp.float32).at[expert_row, column].set(1.0)
    return (row_token_index, row_gate_weights, row_valid_mask)

def reference(tokens, segments, expert_ids, route_weight, norm1_gain, q_weight, kva_weight, kv_gain, kvb_weight, out_weight, norm2_gain, shared_gate, shared_up, shared_down, expert_gate, expert_up_projection, expert_down, cotangent):
    row_token_index, row_gate_weights, row_valid_mask = slot_tables(expert_ids, route_weight)
    blocked = jax.checkpoint(attend)
    expert_layer_apply = jax.checkpoint(experts_one)

    def layer_forward_pass(residual_stream, attention_norm_scale, query_projection_weight, latent_down_weight, latent_norm_scale, latent_up_weight, attention_output_weight, feedforward_norm_scale, shared_gate_weight, shared_up_weight, shared_down_weight, expert_gate_weight, expert_up_weight, expert_down_weight):
        normed_one = low(normalize(residual_stream) * attention_norm_scale)
        mixed_all = lax.map(lambda layer_arguments: blocked(layer_arguments[0], layer_arguments[1], query_projection_weight, latent_down_weight, latent_norm_scale, latent_up_weight), (normed_one.reshape(N_DP, TOK_DEV, D), segments))
        attn_out = low_back(jnp.dot(mixed_all.reshape(TOKENS, H * VDIM), attention_output_weight, precision=highest))
        middle = residual_stream + attn_out
        feedforward_normed_input = low(normalize(middle) * feedforward_norm_scale)
        shared_gate_act = low_back(jnp.dot(feedforward_normed_input, shared_gate_weight, precision=highest))
        shared_up_act = low_back(jnp.dot(feedforward_normed_input, shared_up_weight, precision=highest))
        shared_out = jnp.dot(low(jax.nn.silu(shared_gate_act) * shared_up_act), shared_down_weight, precision=highest)
        expert_routed_rows = lax.map(lambda layer_arguments: expert_layer_apply(feedforward_normed_input, *layer_arguments), (row_token_index, row_gate_weights, row_valid_mask, expert_gate_weight, expert_up_weight, expert_down_weight))
        routed = jnp.zeros((TOKENS, D), jnp.float32).at[row_token_index.reshape(-1)].add(expert_routed_rows.reshape(-1, D))
        return middle + shared_out + routed
    primals = [array_in.astype(jnp.float32) for array_in in (tokens, norm1_gain, q_weight, kva_weight, kv_gain, kvb_weight, out_weight, norm2_gain, shared_gate, shared_up, shared_down, expert_gate, expert_up_projection, expert_down)]
    result, pullback = jax.vjp(layer_forward_pass, *primals)
    gradients = pullback(cotangent.astype(jnp.float32))
    return (result.astype(jnp.bfloat16), gradients[0], gradients[1], gradients[2], gradients[3], gradients[4], gradients[5], gradients[6], gradients[7], gradients[8], gradients[9], gradients[10], gradients[11], gradients[12], gradients[13])
```

```python
import jax
import jax.numpy as jnp
from jax import lax
from jax.sharding import PartitionSpec as P

NOPE = 128
ROPE = 64
VDIM = 128
LATENT = 512
SEGS = 2


epsilon = 1e-06
theta_base = 10000.0


def dot_last(left, right):
    return lax.dot_general(
        left,
        right,
        (((left.ndim - 1,), (right.ndim - 1,)), ((), ())),
        preferred_element_type=jnp.float32,
    )


def dot_first(left, right):
    return lax.dot_general(
        left, right, (((0,), (0,)), ((), ())), preferred_element_type=jnp.float32
    )


def rotate(vector, cosine, sine_part):
    half_width = vector.shape[-1] // 2
    lower_half = vector[..., :half_width]
    upper_half = vector[..., half_width:]
    return jnp.concatenate(
        [
            lower_half * cosine - upper_half * sine_part,
            upper_half * cosine + lower_half * sine_part,
        ],
        axis=-1,
    )


def angles(segment_row):
    seq_len = segment_row.shape[0]
    member = segment_row[:, None] == jnp.arange(SEGS, dtype=jnp.int32)[None, :]
    seq_sizes = jnp.sum(member.astype(jnp.int32), axis=0)
    starts = jnp.cumsum(seq_sizes) - seq_sizes
    seq_first = jnp.sum(jnp.where(member, starts[None, :], 0), axis=1)
    seq_place = (jnp.arange(seq_len, dtype=jnp.int32) - seq_first).astype(jnp.float32)
    inv_freq = theta_base ** (-2.0 * jnp.arange(ROPE // 2, dtype=jnp.float32) / ROPE)
    angle_all = seq_place[:, None] * inv_freq[None, :]
    return (jnp.cos(angle_all), jnp.sin(angle_all))


def norm_scale(vector):
    return lax.rsqrt(jnp.mean(vector * vector, axis=-1, keepdims=True) + epsilon)


def norm_back(grad_hat, hat_value, inv_root):
    return inv_root * (
        grad_hat - hat_value * jnp.mean(grad_hat * hat_value, axis=-1, keepdims=True)
    )


def swish_derivative(grad_act, gate_act, up_act):
    sigma = jax.nn.sigmoid(gate_act)
    return (
        grad_act * up_act * sigma * (1.0 + gate_act * (1.0 - sigma)),
        grad_act * gate_act * sigma,
    )


def slot_tables(ids_all, weights_all, first_expert, local_experts, capacity):
    length = ids_all.shape[2]
    experts = first_expert + jnp.arange(local_experts, dtype=jnp.int32)
    named = ids_all[:, None] == experts[None, :, None, None]
    member = jnp.any(named, axis=2)
    pair_weight = jnp.sum(jnp.where(named, weights_all[:, None], 0.0), axis=2)
    earlier = jnp.arange(length)[:, None] < jnp.arange(length)[None, :]
    rank = jnp.einsum(
        "set,tu->seu",
        member.astype(jnp.bfloat16),
        earlier.astype(jnp.bfloat16),
        preferred_element_type=jnp.float32,
    ).astype(jnp.int32)
    slot = jnp.where(member, rank, -1)
    chosen = slot[:, :, None, :] == jnp.arange(capacity, dtype=jnp.int32)[None, None, :, None]
    slot_weight = jnp.sum(jnp.where(chosen, pair_weight[:, :, None, :], 0.0), axis=3)
    return chosen.astype(jnp.bfloat16), slot_weight


def local(
    tokens,
    segments,
    expert_ids,
    route_weight,
    norm1_gain,
    q_weight,
    kva_weight,
    kv_gain,
    kvb_weight,
    out_weight,
    norm2_gain,
    shared_gate,
    shared_up,
    shared_down,
    expert_gate,
    expert_up_projection,
    expert_down,
    cotangent,
):
    length = tokens.shape[0]
    model_width = tokens.shape[1]
    groups = lax.axis_size("tensor")
    rank_count = lax.axis_size("dp")
    local_experts = expert_gate.shape[0]
    experts_all = local_experts * rank_count
    choose = expert_ids.shape[1]
    capacity = groups * -(-(3 * length * choose) // (2 * experts_all * groups))
    head_count = q_weight.shape[1] // (NOPE + ROPE)
    score_scale = (NOPE + ROPE) ** (-0.5)
    def quarter(rows):
        share = rows.shape[0] // groups
        return lax.dynamic_slice_in_dim(rows, lax.axis_index("tensor") * share, share, 0)

    routing = jnp.concatenate([expert_ids.astype(jnp.float32).T, route_weight.T], axis=0)
    routing_all = lax.all_gather(routing, "dp", axis=0, tiled=False)
    ids_all, weights_all = routing_all[:, :choose], routing_all[:, choose:]
    grad_all = lax.all_gather(quarter(cotangent), ("dp", "tensor"), axis=0, tiled=True)
    query_full, expand_full, output_full, gate_full, lift_full, lower_full = (
        lax.all_gather(q_weight, "dp", axis=0, tiled=True),
        lax.all_gather(kvb_weight, "dp", axis=0, tiled=True),
        lax.all_gather(out_weight, "dp", axis=1, tiled=True),
        lax.all_gather(shared_gate, "dp", axis=0, tiled=True),
        lax.all_gather(shared_up, "dp", axis=0, tiled=True),
        lax.all_gather(shared_down, "dp", axis=1, tiled=True),
    )
    latent_full, attention_norm_scale, latent_norm_scale, feedforward_norm_scale = (
        lax.all_gather(kva_weight, ("dp", "tensor"), axis=0, tiled=True),
        lax.all_gather(norm1_gain, ("dp", "tensor"), axis=0, tiled=True),
        lax.all_gather(kv_gain, ("dp", "tensor"), axis=0, tiled=True),
        lax.all_gather(norm2_gain, ("dp", "tensor"), axis=0, tiled=True),
    )
    attention_norm_scale = attention_norm_scale.astype(jnp.float32)
    latent_norm_scale = latent_norm_scale.astype(jnp.float32)
    feedforward_norm_scale = feedforward_norm_scale.astype(jnp.float32)
    residual_stream = tokens.astype(jnp.float32)
    inv_one = norm_scale(residual_stream)
    hat_one = residual_stream * inv_one
    normed_one = (hat_one * attention_norm_scale).astype(jnp.bfloat16)
    segment_row = segments[0]
    cosine, sine_part = angles(segment_row)
    queries = jnp.dot(normed_one, query_full, preferred_element_type=jnp.float32).reshape(
        length, head_count, NOPE + ROPE
    )
    q_rot = jnp.concatenate(
        [
            queries[..., :NOPE],
            rotate(queries[..., NOPE:], cosine[:, None, :], sine_part[:, None, :]),
        ],
        axis=-1,
    ).astype(jnp.bfloat16)
    compressed = jnp.dot(normed_one, latent_full, preferred_element_type=jnp.float32)
    latent_raw = compressed[:, :LATENT]
    inv_kv = norm_scale(latent_raw)
    hat_kv = latent_raw * inv_kv
    latent_low = (hat_kv * latent_norm_scale).astype(jnp.bfloat16)
    key_rot = rotate(compressed[:, LATENT:], cosine, sine_part).astype(jnp.bfloat16)
    keyval = (
        jnp.dot(latent_low, expand_full, preferred_element_type=jnp.float32)
        .astype(jnp.bfloat16)
        .reshape(length, head_count, NOPE + VDIM)
    )
    key_nope = keyval[..., :NOPE]
    values = keyval[..., NOPE:]
    positions = jnp.arange(length, dtype=jnp.int32)
    allowed = (segment_row[:, None] == segment_row[None, :]) & (
        positions[None, :] <= positions[:, None]
    )

    def raw_scores():
        dots = jnp.einsum(
            "thd,shd->hts", q_rot[..., :NOPE], key_nope, preferred_element_type=jnp.float32
        )
        dots = dots + jnp.einsum(
            "thr,sr->hts", q_rot[..., NOPE:], key_rot, preferred_element_type=jnp.float32
        )
        return jnp.where(allowed[None], dots * score_scale, -1000000000.0)

    scores = raw_scores()
    row_peak = jnp.max(scores, axis=-1, keepdims=True)
    log_total = jnp.log(jnp.sum(jnp.exp(scores - row_peak), axis=-1, keepdims=True)) + row_peak
    attn_probs = jnp.exp(scores - log_total)
    mixed_heads = (
        jnp.einsum(
            "hts,shv->thv",
            attn_probs.astype(jnp.bfloat16),
            values,
            preferred_element_type=jnp.float32,
        )
        .astype(jnp.bfloat16)
        .reshape(length, head_count * VDIM)
    )
    attn_out = lax.psum(
        jnp.dot(mixed_heads, output_full, preferred_element_type=jnp.float32).astype(jnp.bfloat16),
        "tensor",
    ).astype(jnp.float32)
    middle = residual_stream + attn_out
    inv_two = norm_scale(middle)
    hat_two = middle * inv_two
    feedforward_normed_input = (hat_two * feedforward_norm_scale).astype(jnp.bfloat16)
    shared_gate_act = jnp.dot(
        feedforward_normed_input, gate_full, preferred_element_type=jnp.float32
    )
    shared_up_act = jnp.dot(feedforward_normed_input, lift_full, preferred_element_type=jnp.float32)
    shared_hidden = (jax.nn.silu(shared_gate_act) * shared_up_act).astype(jnp.bfloat16)
    shared_out = jnp.dot(shared_hidden, lower_full, preferred_element_type=jnp.float32)
    first_expert = lax.axis_index("dp") * local_experts
    chosen, slot_weight = slot_tables(
        ids_all.astype(jnp.int32), weights_all, first_expert, local_experts, capacity
    )
    rows_all = lax.all_gather(quarter(feedforward_normed_input), ("dp", "tensor"), axis=0, tiled=True)
    received_rows = jnp.einsum(
        "sect,std->secd",
        chosen,
        rows_all.reshape(rank_count, length, model_width),
        preferred_element_type=jnp.float32,
    ).astype(jnp.bfloat16)
    grad_arrived = jnp.einsum(
        "sect,std->secd",
        chosen,
        grad_all.reshape(rank_count, length, model_width),
        preferred_element_type=jnp.float32,
    )
    grad_arrived = (grad_arrived * slot_weight[..., None]).astype(jnp.bfloat16)
    expert_gate_activation = jnp.einsum(
        "secd,edf->secf", received_rows, expert_gate, preferred_element_type=jnp.float32
    )
    expert_up_activation = jnp.einsum(
        "secd,edf->secf", received_rows, expert_up_projection, preferred_element_type=jnp.float32
    )
    expert_hidden = (jax.nn.silu(expert_gate_activation) * expert_up_activation).astype(
        jnp.bfloat16
    )
    expert_out = jnp.einsum(
        "secf,efd->secd", expert_hidden, expert_down, preferred_element_type=jnp.float32
    )
    expert_out = (expert_out * slot_weight[..., None]).astype(jnp.bfloat16)
    routed = jnp.einsum(
        "sect,secd->std", chosen, expert_out, preferred_element_type=jnp.float32
    ).astype(jnp.bfloat16)
    routed = lax.psum_scatter(
        routed.reshape(rank_count * length, model_width), "dp", scatter_dimension=0, tiled=True
    ).astype(jnp.float32)
    block_out = lax.psum((shared_out + routed).astype(jnp.bfloat16), "tensor").astype(jnp.float32)
    output = (middle + block_out).astype(jnp.bfloat16)
    grad_out = cotangent.astype(jnp.float32)
    hidden_state_gradient = jnp.einsum(
        "secd,efd->secf", grad_arrived, expert_down, preferred_element_type=jnp.float32
    )
    grad_expert_down = jnp.einsum(
        "secf,secd->efd", expert_hidden, grad_arrived, preferred_element_type=jnp.float32
    )
    expert_gate_gradient, expert_up_gradient = swish_derivative(
        hidden_state_gradient, expert_gate_activation, expert_up_activation
    )
    expert_gate_gradient = expert_gate_gradient.astype(jnp.bfloat16)
    expert_up_gradient = expert_up_gradient.astype(jnp.bfloat16)
    grad_expert_gate = jnp.einsum(
        "zxmi,zxmh->xih", received_rows, expert_gate_gradient, preferred_element_type=jnp.float32
    )
    grad_expert_up = jnp.einsum(
        "zxmi,zxmh->xih", received_rows, expert_up_gradient, preferred_element_type=jnp.float32
    )
    grad_inputs = jnp.einsum(
        "azlh,zoh->azlo", expert_gate_gradient, expert_gate, preferred_element_type=jnp.float32
    )
    grad_inputs = (
        grad_inputs
        + jnp.einsum(
            "azlh,zoh->azlo",
            expert_up_gradient,
            expert_up_projection,
            preferred_element_type=jnp.float32,
        )
    ).astype(jnp.bfloat16)
    routed_grad = jnp.einsum(
        "sect,secd->std", chosen, grad_inputs, preferred_element_type=jnp.float32
    ).astype(jnp.bfloat16)
    routed_grad = lax.psum_scatter(
        routed_grad.reshape(rank_count * length, model_width), "dp", scatter_dimension=0, tiled=True
    ).astype(jnp.float32)
    grad_shared_hidden = dot_last(cotangent, lower_full)
    grad_sgate, grad_sup = swish_derivative(grad_shared_hidden, shared_gate_act, shared_up_act)
    grad_sgate = grad_sgate.astype(jnp.bfloat16)
    grad_sup = grad_sup.astype(jnp.bfloat16)
    grad_lower = dot_first(shared_hidden, cotangent)
    grad_gate_full = dot_first(feedforward_normed_input, grad_sgate)
    grad_lift_full = dot_first(feedforward_normed_input, grad_sup)
    grad_normed_two = dot_last(grad_sgate, gate_full) + dot_last(grad_sup, lift_full) + routed_grad
    grad_normed_two = lax.psum(grad_normed_two.astype(jnp.bfloat16), "tensor").astype(jnp.float32)
    token_share = length // groups
    share_start = lax.axis_index("tensor") * token_share
    grad_gain_two = jnp.sum(
        lax.dynamic_slice_in_dim(grad_normed_two * hat_two, share_start, token_share, 0), axis=0
    )
    grad_middle = grad_out + norm_back(grad_normed_two * feedforward_norm_scale, hat_two, inv_two)
    grad_middle_low = grad_middle.astype(jnp.bfloat16)
    grad_output_full = dot_first(mixed_heads, grad_middle_low)
    grad_mixed = (
        dot_last(grad_middle_low, output_full)
        .astype(jnp.bfloat16)
        .reshape(length, head_count, VDIM)
    )
    scores = raw_scores()
    attn_probs = jnp.exp(scores - log_total)
    grad_probs = jnp.einsum("thv,shv->hts", grad_mixed, values, preferred_element_type=jnp.float32)
    grad_values = jnp.einsum(
        "hts,thv->shv",
        attn_probs.astype(jnp.bfloat16),
        grad_mixed,
        preferred_element_type=jnp.float32,
    )
    row_delta = jnp.sum(attn_probs * grad_probs, axis=-1, keepdims=True)
    grad_scores = (attn_probs * (grad_probs - row_delta)).astype(jnp.bfloat16)
    grad_q_nope = (
        jnp.einsum("hts,shd->thd", grad_scores, key_nope, preferred_element_type=jnp.float32)
        * score_scale
    )
    grad_q_rope = (
        jnp.einsum("hts,sr->thr", grad_scores, key_rot, preferred_element_type=jnp.float32)
        * score_scale
    )
    grad_k_nope = (
        jnp.einsum(
            "hts,thd->shd", grad_scores, q_rot[..., :NOPE], preferred_element_type=jnp.float32
        )
        * score_scale
    )
    grad_k_rope = (
        jnp.einsum(
            "hts,thr->sr", grad_scores, q_rot[..., NOPE:], preferred_element_type=jnp.float32
        )
        * score_scale
    )
    grad_queries = jnp.concatenate(
        [grad_q_nope, rotate(grad_q_rope, cosine[:, None, :], -sine_part[:, None, :])], axis=-1
    )
    grad_queries = grad_queries.astype(jnp.bfloat16).reshape(length, head_count * (NOPE + ROPE))
    grad_keyval = (
        jnp.concatenate([grad_k_nope, grad_values], axis=-1)
        .astype(jnp.bfloat16)
        .reshape(length, head_count * (NOPE + VDIM))
    )
    grad_query_full = dot_first(normed_one, grad_queries)
    grad_expand_full = dot_first(latent_low, grad_keyval)
    grad_latent = dot_last(grad_keyval, expand_full)
    grad_gain_kv = jnp.sum(grad_latent * hat_kv, axis=0)
    grad_latent_raw = norm_back(grad_latent * latent_norm_scale, hat_kv, inv_kv)
    grad_compressed = jnp.concatenate(
        [grad_latent_raw, rotate(grad_k_rope, cosine, -sine_part)], axis=-1
    ).astype(jnp.bfloat16)
    grad_latent_full = dot_first(normed_one, grad_compressed)
    grad_normed_one = dot_last(grad_queries, query_full) + dot_last(grad_compressed, latent_full)
    grad_normed_one = lax.psum(grad_normed_one.astype(jnp.bfloat16), "tensor").astype(jnp.float32)
    grad_gain_one = jnp.sum(
        lax.dynamic_slice_in_dim(grad_normed_one * hat_one, share_start, token_share, 0), axis=0
    )
    grad_tokens = grad_middle + norm_back(grad_normed_one * attention_norm_scale, hat_one, inv_one)
    (
        grad_q_weight,
        grad_kvb_weight,
        grad_out_weight,
        grad_shared_gate,
        grad_shared_up,
        grad_shared_down,
    ) = (
        lax.psum_scatter(
            grad_query_full.astype(jnp.bfloat16), "dp", scatter_dimension=0, tiled=True
        ).astype(jnp.float32),
        lax.psum_scatter(
            grad_expand_full.astype(jnp.bfloat16), "dp", scatter_dimension=0, tiled=True
        ).astype(jnp.float32),
        lax.psum_scatter(
            grad_output_full.astype(jnp.bfloat16), "dp", scatter_dimension=1, tiled=True
        ).astype(jnp.float32),
        lax.psum_scatter(
            grad_gate_full.astype(jnp.bfloat16), "dp", scatter_dimension=0, tiled=True
        ).astype(jnp.float32),
        lax.psum_scatter(
            grad_lift_full.astype(jnp.bfloat16), "dp", scatter_dimension=0, tiled=True
        ).astype(jnp.float32),
        lax.psum_scatter(
            grad_lower.astype(jnp.bfloat16), "dp", scatter_dimension=1, tiled=True
        ).astype(jnp.float32),
    )
    grad_kva_weight, grad_norm1_gain, grad_kv_gain, grad_norm2_gain = (
        lax.psum_scatter(grad_latent_full, ("dp", "tensor"), scatter_dimension=0, tiled=True),
        lax.psum_scatter(grad_gain_one, ("dp", "tensor"), scatter_dimension=0, tiled=True),
        lax.psum_scatter(grad_gain_kv, ("dp", "tensor"), scatter_dimension=0, tiled=True),
        lax.psum_scatter(grad_gain_two, ("dp", "tensor"), scatter_dimension=0, tiled=True),
    )
    return (
        output,
        grad_tokens,
        grad_norm1_gain,
        grad_q_weight,
        grad_kva_weight,
        grad_kv_gain,
        grad_kvb_weight,
        grad_out_weight,
        grad_norm2_gain,
        grad_shared_gate,
        grad_shared_up,
        grad_shared_down,
        grad_expert_gate,
        grad_expert_up,
        grad_expert_down,
    )


def solution(mesh):
    in_specs = (
        P("dp", None),
        P("dp", None),
        P("dp", None),
        P("dp", None),
        P(("dp", "tensor")),
        P("dp", "tensor"),
        P(("dp", "tensor"), None),
        P(("dp", "tensor")),
        P("dp", "tensor"),
        P("tensor", "dp"),
        P(("dp", "tensor")),
        P("dp", "tensor"),
        P("dp", "tensor"),
        P("tensor", "dp"),
        P("dp", None, "tensor"),
        P("dp", None, "tensor"),
        P("dp", "tensor", None),
        P("dp", None),
    )
    out_specs = (
        P("dp", None),
        P("dp", None),
        P(("dp", "tensor")),
        P("dp", "tensor"),
        P(("dp", "tensor"), None),
        P(("dp", "tensor")),
        P("dp", "tensor"),
        P("tensor", "dp"),
        P(("dp", "tensor")),
        P("dp", "tensor"),
        P("dp", "tensor"),
        P("tensor", "dp"),
        P("dp", None, "tensor"),
        P("dp", None, "tensor"),
        P("dp", "tensor", None),
    )
    return jax.shard_map(local, mesh=mesh, in_specs=in_specs, out_specs=out_specs, check_vma=False)
```

```python
import functools

import jax
import jax.numpy as jnp
from jax import lax
from jax.experimental import pallas as pl
from jax.experimental.pallas import tpu as pltpu
from jax.sharding import PartitionSpec as P


NOPE = 128
ROPE = 64
VDIM = 128
LATENT = 512
SEGS = 2


DP, TP = "dp", "tensor"
epsilon = 1e-06
theta_base = 10000.0


def dot_last(left, right):
    return lax.dot_general(
        left,
        right,
        (((left.ndim - 1,), (right.ndim - 1,)), ((), ())),
        preferred_element_type=jnp.float32,
    )


def dot_first(left, right):
    return lax.dot_general(
        left, right, (((0,), (0,)), ((), ())), preferred_element_type=jnp.float32
    )


def rotate(vector, cosine, sine_part):
    half_width = vector.shape[-1] // 2
    lower_half = vector[..., :half_width]
    upper_half = vector[..., half_width:]
    return jnp.concatenate(
        [
            lower_half * cosine - upper_half * sine_part,
            upper_half * cosine + lower_half * sine_part,
        ],
        axis=-1,
    )


def angles(segment_row):
    seq_len = segment_row.shape[0]
    member = segment_row[:, None] == jnp.arange(SEGS, dtype=jnp.int32)[None, :]
    seq_sizes = jnp.sum(member.astype(jnp.int32), axis=0)
    starts = jnp.cumsum(seq_sizes) - seq_sizes
    seq_first = jnp.sum(jnp.where(member, starts[None, :], 0), axis=1)
    seq_place = (jnp.arange(seq_len, dtype=jnp.int32) - seq_first).astype(jnp.float32)
    inv_freq = theta_base ** (-2.0 * jnp.arange(ROPE // 2, dtype=jnp.float32) / ROPE)
    angle_all = seq_place[:, None] * inv_freq[None, :]
    return (jnp.cos(angle_all), jnp.sin(angle_all))


def norm_scale(vector):
    return lax.rsqrt(jnp.mean(vector * vector, axis=-1, keepdims=True) + epsilon)


def norm_back(grad_hat, hat_value, inv_root):
    return inv_root * (
        grad_hat - hat_value * jnp.mean(grad_hat * hat_value, axis=-1, keepdims=True)
    )


def swish_derivative(grad_act, gate_act, up_act):
    sigma = jax.nn.sigmoid(gate_act)
    return (
        grad_act * up_act * sigma * (1.0 + gate_act * (1.0 - sigma)),
        grad_act * gate_act * sigma,
    )


def after(value, *earlier):
    if not earlier:
        return value
    return lax.optimization_barrier((value,) + earlier)[0]


def shift_tensor(value, step):
    size = lax.axis_size(TP)
    return lax.ppermute(value, TP, [(i, (i + step) % size) for i in range(size)])


def shift_chips(value, step):
    chips = lax.axis_size(DP) // 2
    pairs = [(2 * z + c, 2 * ((z + step) % chips) + c) for z in range(chips) for c in range(2)]
    return lax.ppermute(value, DP, pairs)


def swap_cores(value):
    return lax.ppermute(value, DP, [(i, i ^ 1) for i in range(lax.axis_size(DP))])


def pick(value, index, axis=0):
    return lax.dynamic_index_in_dim(value, index, axis, keepdims=False)


def place(pieces, owners, hold=()):
    whole = after(jnp.zeros((len(pieces),) + pieces[0].shape, pieces[0].dtype), *hold)
    for piece, owner in zip(pieces, owners):
        whole = lax.dynamic_update_index_in_dim(whole, piece, owner, 0)
    return whole


def gather_dp(value, hold=()):
    ranks = lax.axis_size(DP)
    chips = ranks // 2
    index = lax.axis_index(DP)
    core, chip = index % 2, index // 2
    mine = [value] + [shift_chips(value, k) for k in range(1, chips)]
    other = [swap_cores(piece) for piece in mine]
    origin = [(chip - k) % chips for k in range(chips)]
    owners = [2 * z + core for z in origin] + [2 * z + 1 - core for z in origin]
    return place(mine + other, owners, hold)


def gather_tensor(value):
    size = lax.axis_size(TP)
    index = lax.axis_index(TP)
    pieces = [value] + [shift_tensor(value, j) for j in range(1, size)]
    whole = place(pieces, [(index - j) % size for j in range(size)])
    return whole.reshape((size * value.shape[0],) + value.shape[1:])


def total(pieces):
    whole = pieces[0].astype(jnp.float32)
    for piece in pieces[1:]:
        whole = whole + piece.astype(jnp.float32)
    return whole


def scatter_tensor(value):
    size = lax.axis_size(TP)
    index = lax.axis_index(TP)
    value = value.reshape((size, value.shape[0] // size) + value.shape[1:])
    pieces = [shift_tensor(pick(value, (index + j) % size), j) for j in range(1, size)]
    return total([pick(value, index)] + pieces)


def shift_outer(value, step):
    size = lax.axis_size(TP)
    inner = size // 2
    pairs = [(i, (i + step * inner) % size) for i in range(size)]
    return lax.ppermute(value, TP, pairs)


def shift_inner(value, step):
    size = lax.axis_size(TP)
    inner = size // 2
    pairs = [(i, i // inner * inner + (i + step) % inner) for i in range(size)]
    return lax.ppermute(value, TP, pairs)


def scatter_half(held, inner_first, hold_first, hold_second, hold_last):
    inner = len(held) // 2
    chips, dtype = held[0].shape[0], held[0].dtype
    if inner_first:
        groups = [[held[o * inner + i] for i in range(inner)] for o in range(2)]
        first, second = shift_inner, shift_outer
    else:
        groups = [[held[o * inner + i] for o in range(2)] for i in range(inner)]
        first, second = shift_outer, shift_inner
    moved = [[first(group[n], n) for n in range(1, len(group))] for group in groups]
    sums = [
        total([after(group[0], *hold_first)] + arrived).astype(dtype)
        for group, arrived in zip(groups, moved)
    ]
    moved = [second(sums[n], n) for n in range(1, len(sums))]
    kept = after(sums[0], *hold_second)
    pieces = [total([kept[k]] + [piece[k] for piece in moved]).astype(dtype) for k in range(chips)]
    moved = [shift_chips(pieces[k], k) for k in range(1, chips)]
    return total([after(pieces[0], *hold_last)] + moved)


def scatter_all(held, hold_first=(), hold_second=(), hold_last=()):
    return jnp.concatenate(
        [
            scatter_half(half, n == 0, hold_first, hold_second, hold_last)
            for n, half in enumerate(held)
        ],
        axis=1,
    )


def scatter_small(value, hold):
    ranks, size = lax.axis_size(DP), lax.axis_size(TP)
    index, column = lax.axis_index(DP), lax.axis_index(TP)
    core, chip = index % 2, index // 2
    value = value.reshape(ranks // 2, 2, size, value.shape[-1])
    value = pick(value, core, 1) + swap_cores(pick(value, 1 - core, 1))
    pieces = [shift_tensor(pick(value, (column + j) % size, 1), j) for j in range(1, size)]
    value = total([pick(value, column, 1)] + pieces)
    value = after(value, *hold)
    pieces = [shift_chips(pick(value, (chip + k) % (ranks // 2)), k) for k in range(1, ranks // 2)]
    return total([pick(value, chip)] + pieces)


def slot_tables(ids_all, weights_all, first_expert, local_experts, capacity):
    length = ids_all.shape[2]
    experts = first_expert + jnp.arange(local_experts, dtype=jnp.int32)
    named = ids_all[:, None] == experts[None, :, None, None]
    member = jnp.any(named, axis=2)
    pair_weight = jnp.sum(jnp.where(named, weights_all[:, None], 0.0), axis=2)
    earlier = jnp.arange(length)[:, None] < jnp.arange(length)[None, :]
    rank = jnp.einsum(
        "set,tu->seu",
        member.astype(jnp.bfloat16),
        earlier.astype(jnp.bfloat16),
        preferred_element_type=jnp.float32,
    ).astype(jnp.int32)
    slot = jnp.where(member, rank, -1)
    chosen = slot[:, :, None, :] == jnp.arange(capacity, dtype=jnp.int32)[None, None, :, None]
    slot_weight = jnp.sum(jnp.where(chosen, pair_weight[:, :, None, :], 0.0), axis=3)
    slot_token = jnp.sum(
        jnp.where(chosen, jnp.arange(length, dtype=jnp.int32) + 1, 0), axis=3
    ) - 1
    return slot_token, slot_weight


def fetch_kernel(token_ref, rows_ref, out_ref):
    experts, room = out_ref.shape[:2]
    slots, length = token_ref.shape[0], rows_ref.shape[0]
    position = lax.broadcasted_iota(jnp.int32, (slots, length), 1)
    chosen = (token_ref[...] == position).astype(jnp.bfloat16)
    fetched = jnp.dot(chosen, rows_ref[...], preferred_element_type=jnp.float32)
    fetched = fetched.astype(jnp.bfloat16)
    for e in range(experts):
        out_ref[e] = fetched[e * room : (e + 1) * room]


def fetch_rows(slot_token, rows):
    ranks, experts, room = slot_token.shape
    length, width = rows.shape[1:]
    slots = experts * room
    return pl.pallas_call(
        fetch_kernel,
        grid=(ranks,),
        in_specs=[
            pl.BlockSpec((None, slots, 1), lambda s: (s, 0, 0)),
            pl.BlockSpec((None, length, width), lambda s: (s, 0, 0)),
        ],
        out_specs=pl.BlockSpec((experts, room, width), lambda s: (0, s, 0)),
        out_shape=jax.ShapeDtypeStruct((experts, ranks * room, width), jnp.bfloat16),
        cost_estimate=pl.CostEstimate(
            flops=2 * ranks * slots * length * width,
            bytes_accessed=2 * ranks * (slots + length) * width,
            transcendentals=0,
        ),
        name="fetch_rows",
    )(slot_token.reshape(ranks, slots, 1), rows)


def return_kernel(with_extra, order_ref, start_ref, token_ref, rows_ref, *refs):
    experts, room, width = rows_ref.shape
    extra_ref, refs = (refs[0], refs[1:]) if with_extra else (None, refs)
    size, count = start_ref.shape[0], refs[0].shape[0]
    arrived_refs, out_refs = refs[: -2 * size], refs[-2 * size :]
    rows = rows_ref[...].reshape(experts * room, width)
    position = lax.broadcasted_iota(jnp.int32, (count, experts * room), 0)
    for step in range(size):
        chosen = (token_ref[...] == position + step * count).astype(jnp.bfloat16)
        sums = jnp.dot(chosen, rows, preferred_element_type=jnp.float32)
        if with_extra:
            begin = pl.multiple_of(start_ref[step] * count, count)
            extra = extra_ref[pl.ds(begin, count)].astype(jnp.float32)
            sums = sums + jnp.where(pl.program_id(0) == 0, extra, 0.0)
        for half in range(2):
            part = sums[:, half * (width // 2) : (half + 1) * (width // 2)]
            if arrived_refs:
                part = part + arrived_refs[half * size + step][...].astype(jnp.float32)
            out_refs[half * size + step][...] = part.astype(jnp.bfloat16)


def return_rows(order, starts, slot_token, rows, length, extra=None, arrived=None):
    steps, (ranks, experts, room), width = order.shape[0], slot_token.shape, rows.shape[2]
    size, slots = starts.shape[0], experts * room
    count = length // size
    more = [] if extra is None else [extra]
    more_specs = [] if extra is None else [pl.BlockSpec((length, width), lambda k, o, s: (0, 0))]
    cut_specs = [pl.BlockSpec((None, count, width // 2), lambda k, o, s: (k, 0, 0))] * (2 * size)
    if arrived is not None:
        more = more + list(arrived[0]) + list(arrived[1])
        more_specs = more_specs + cut_specs
    results = pl.pallas_call(
        functools.partial(return_kernel, extra is not None),
        grid_spec=pltpu.PrefetchScalarGridSpec(
            num_scalar_prefetch=2,
            grid=(steps,),
            in_specs=[
                pl.BlockSpec((None, 1, slots), lambda k, o, s: (o[k], 0, 0)),
                pl.BlockSpec((experts, room, width), lambda k, o, s: (0, o[k], 0)),
            ]
            + more_specs,
            out_specs=cut_specs,
        ),
        out_shape=[jax.ShapeDtypeStruct((steps, count, width // 2), jnp.bfloat16)] * (2 * size),
        cost_estimate=pl.CostEstimate(
            flops=2 * steps * slots * length * width,
            bytes_accessed=2 * steps * (slots + 2 * length) * width,
            transcendentals=0,
        ),
        name="return_rows",
    )(order, starts, slot_token.reshape(ranks, 1, slots), rows, *more)
    return results[:size], results[size:]


def expert_kernel(
    rows_ref, grad_ref, weight_ref, slot_ref, back_ref, hidden_ref, scaled_ref, gate_ref, up_ref, both
):
    width = grad_ref.shape[1]
    half = weight_ref.shape[1] // 2

    @pl.when((pl.program_id(0) == 0) & (pl.program_id(1) == 0))
    def _():
        both[...] = jnp.zeros_like(both)

    acts = jnp.dot(rows_ref[...], weight_ref[...], preferred_element_type=jnp.float32)
    gate_act, up_act = acts[:, :width], acts[:, half : half + width]
    sigma = 1.0 / (1.0 + jnp.exp(-gate_act))
    silu = gate_act * sigma
    hidden = (silu * up_act).astype(jnp.bfloat16)
    hidden_ref[...] = hidden
    scaled_ref[...] = (hidden.astype(jnp.float32) * slot_ref[...]).astype(jnp.bfloat16)
    grad = grad_ref[...] * slot_ref[...]
    gate_grad = (grad * up_act * sigma * (1.0 + gate_act * (1.0 - sigma))).astype(jnp.bfloat16)
    up_grad = (grad * silu).astype(jnp.bfloat16)
    gate_ref[...] = gate_grad
    up_ref[...] = up_grad
    both[:, :width] = gate_grad
    both[:, half : half + width] = up_grad
    back_ref[...] = lax.dot_general(
        both[...], weight_ref[...], (((1,), (1,)), ((), ())), preferred_element_type=jnp.float32
    ).astype(jnp.bfloat16)


def expert_pass(rows, grad_hidden, weights, slot_weight):
    experts, slots, width = rows.shape
    hidden = grad_hidden.shape[2]
    share = slots // 2
    row_spec = pl.BlockSpec((None, share, width), lambda e, i: (e, i, 0))
    hidden_spec = pl.BlockSpec((None, share, hidden), lambda e, i: (e, i, 0))
    hidden_shape = jax.ShapeDtypeStruct((experts, slots, hidden), jnp.bfloat16)
    return pl.pallas_call(
        expert_kernel,
        grid=(experts, 2),
        in_specs=[
            row_spec,
            hidden_spec,
            pl.BlockSpec((None,) + weights.shape[1:], lambda e, i: (e, 0, 0)),
            pl.BlockSpec((None, share, 1), lambda e, i: (e, i, 0)),
        ],
        out_specs=[row_spec] + [hidden_spec] * 4,
        out_shape=[jax.ShapeDtypeStruct(rows.shape, jnp.bfloat16)] + [hidden_shape] * 4,
        scratch_shapes=[pltpu.VMEM((share, weights.shape[2]), jnp.bfloat16)],
        cost_estimate=pl.CostEstimate(
            flops=8 * experts * slots * width * hidden,
            bytes_accessed=4 * experts * (slots + hidden) * width,
            transcendentals=experts * slots * hidden,
        ),
        name="expert_pass",
    )(rows, grad_hidden, weights, slot_weight[..., None])


def side_by_side(value, ranks):
    width = value.shape[1]
    value = value.reshape(ranks, 4, -1, width).transpose(0, 2, 1, 3)
    return value.reshape(-1, 4 * width)


def stacked(value, ranks):
    width = value.shape[1] // 4
    value = value.reshape(ranks, -1, 4, width).transpose(0, 2, 1, 3)
    return value.reshape(-1, width)


def local(
    tokens,
    segments,
    expert_ids,
    route_weight,
    norm1_gain,
    q_weight,
    kva_weight,
    kv_gain,
    kvb_weight,
    out_weight,
    norm2_gain,
    shared_gate,
    shared_up,
    shared_down,
    expert_gate,
    expert_up_projection,
    expert_down,
    cotangent,
):
    length = tokens.shape[0]
    model_width = tokens.shape[1]
    groups = lax.axis_size(TP)
    rank_count = lax.axis_size(DP)
    local_experts = expert_gate.shape[0]
    experts_all = local_experts * rank_count
    choose = expert_ids.shape[1]
    capacity = groups * -(-(3 * length * choose) // (2 * experts_all * groups))
    slot_room = 16 * -(-capacity // 16)
    head_count = q_weight.shape[1] // (NOPE + ROPE)
    score_scale = (NOPE + ROPE) ** (-0.5)
    dp_index = lax.axis_index(DP)
    column = lax.axis_index(TP)
    chips = rank_count // 2
    token_share = length // groups

    def quarter(rows):
        return lax.dynamic_slice_in_dim(rows, column * token_share, token_share, 0)

    gain_widths = (norm1_gain.shape[0], kv_gain.shape[0], norm2_gain.shape[0])
    latent_rows, latent_width = kva_weight.shape
    gain_row = jnp.concatenate([norm1_gain, kv_gain, norm2_gain])
    gain_columns = -(-sum(gain_widths) // latent_rows)
    gain_row = jnp.pad(gain_row, (0, gain_columns * latent_rows - sum(gain_widths)))
    small = jnp.concatenate([kva_weight, gain_row.reshape(latent_rows, gain_columns)], axis=1)
    small = gather_dp(small)
    pieces = [small] + [shift_tensor(small, j) for j in range(1, groups)]
    pieces = tuple(pieces)
    small_all = jnp.zeros((rank_count, groups) + small.shape[1:], small.dtype)
    for j, piece in enumerate(pieces):
        small_all = lax.dynamic_update_index_in_dim(small_all, piece, (column - j) % groups, 1)
    small_all = small_all.reshape(-1, latent_width + gain_columns)
    latent_full = small_all[:, :latent_width]
    gains_all = small_all[:, latent_width:].reshape(rank_count * groups, -1).astype(jnp.float32)
    attention_norm_scale = gains_all[:, : gain_widths[0]].reshape(-1)
    latent_norm_scale = gains_all[:, gain_widths[0] : gain_widths[0] + gain_widths[1]].reshape(-1)
    feedforward_norm_scale = gains_all[:, gain_widths[0] + gain_widths[1] : sum(gain_widths)].reshape(-1)

    expand_full = gather_dp(kvb_weight, pieces).reshape(-1, kvb_weight.shape[1])
    query_full = gather_dp(q_weight, pieces).reshape(-1, q_weight.shape[1])
    output_rows = gather_dp(after(out_weight, small_all))
    output_full = output_rows.transpose(1, 0, 2).reshape(out_weight.shape[0], -1)

    routing = jnp.concatenate([expert_ids.astype(jnp.float32).T, route_weight.T], axis=0)
    routing_all = gather_dp(routing)
    ids_all, weights_all = routing_all[:, :choose].astype(jnp.int32), routing_all[:, choose:]
    grad_all = lax.all_gather(
        quarter(cotangent), (DP, TP), axis=0, tiled=True
    )
    residual_stream = tokens.astype(jnp.float32)
    inv_one = norm_scale(residual_stream)
    hat_one = residual_stream * inv_one
    normed_one = (hat_one * attention_norm_scale).astype(jnp.bfloat16)
    segment_row = segments[0]
    cosine, sine_part = angles(segment_row)
    queries = jnp.dot(normed_one, query_full, preferred_element_type=jnp.float32).reshape(
        length, head_count, NOPE + ROPE
    )
    q_rot = jnp.concatenate(
        [
            queries[..., :NOPE],
            rotate(queries[..., NOPE:], cosine[:, None, :], sine_part[:, None, :]),
        ],
        axis=-1,
    ).astype(jnp.bfloat16)
    compressed = jnp.dot(normed_one, latent_full, preferred_element_type=jnp.float32)
    latent_raw = compressed[:, :LATENT]
    inv_kv = norm_scale(latent_raw)
    hat_kv = latent_raw * inv_kv
    latent_low = (hat_kv * latent_norm_scale).astype(jnp.bfloat16)
    key_rot = rotate(compressed[:, LATENT:], cosine, sine_part).astype(jnp.bfloat16)
    keyval = (
        jnp.dot(latent_low, expand_full, preferred_element_type=jnp.float32)
        .astype(jnp.bfloat16)
        .reshape(length, head_count, NOPE + VDIM)
    )
    key_nope = keyval[..., :NOPE]
    values = keyval[..., NOPE:]
    positions = jnp.arange(length, dtype=jnp.int32)
    allowed = (segment_row[:, None] == segment_row[None, :]) & (
        positions[None, :] <= positions[:, None]
    )

    def raw_scores():
        dots = jnp.einsum(
            "thd,shd->hts", q_rot[..., :NOPE], key_nope, preferred_element_type=jnp.float32
        )
        dots = dots + jnp.einsum(
            "thr,sr->hts", q_rot[..., NOPE:], key_rot, preferred_element_type=jnp.float32
        )
        return jnp.where(allowed[None], dots * score_scale, -1000000000.0)

    scores = raw_scores()
    row_peak = jnp.max(scores, axis=-1, keepdims=True)
    log_total = jnp.log(jnp.sum(jnp.exp(scores - row_peak), axis=-1, keepdims=True)) + row_peak
    attn_probs = jnp.exp(scores - log_total)
    mixed_heads = (
        jnp.einsum(
            "hts,shv->thv",
            attn_probs.astype(jnp.bfloat16),
            values,
            preferred_element_type=jnp.float32,
        )
        .astype(jnp.bfloat16)
        .reshape(length, head_count * VDIM)
    )
    attn_out = scatter_tensor(
        jnp.dot(mixed_heads, output_full, preferred_element_type=jnp.float32).astype(jnp.bfloat16)
    )
    middle = quarter(tokens).astype(jnp.float32) + after(attn_out, grad_all)
    inv_two = norm_scale(middle)
    hat_two = middle * inv_two
    normed_two = (hat_two * feedforward_norm_scale).astype(jnp.bfloat16)
    rows_all = lax.all_gather(normed_two, (DP, TP), axis=0, tiled=True)
    feedforward_normed_input = lax.dynamic_slice_in_dim(rows_all, dp_index * length, length, 0)

    gate_lift_full = lax.all_gather(
        jnp.concatenate([shared_gate, shared_up], axis=1), DP, axis=0, tiled=True
    )
    lower_full = lax.all_gather(shared_down, DP, axis=1, tiled=True)

    slot_token, slot_weight = slot_tables(
        ids_all, weights_all, dp_index * local_experts, local_experts, slot_room
    )
    inner = groups // 2
    share = slot_token // token_share
    step = (share // inner - column // inner) % 2 * inner + (share - column) % inner
    outer_steps = jnp.arange(groups, dtype=jnp.int32) // inner
    inner_steps = jnp.arange(groups, dtype=jnp.int32) % inner
    step_starts = (column // inner + outer_steps) % 2 * inner + (column + inner_steps) % inner
    near_token = jnp.where(slot_token < 0, -1, step * token_share + slot_token % token_share)
    slot_weight = slot_weight.transpose(1, 0, 2).reshape(local_experts, -1)
    chip_steps = (dp_index // 2 + jnp.arange(chips, dtype=jnp.int32)) % chips
    own_order = 2 * chip_steps + dp_index % 2
    other_order = 2 * chip_steps + 1 - dp_index % 2
    expert_width = expert_gate.shape[2]
    lane_pad = ((0, 0), (0, 0), (0, -expert_width % 128))
    gate_up = jnp.concatenate(
        [jnp.pad(expert_gate, lane_pad), jnp.pad(expert_up_projection, lane_pad)], axis=2
    )
    grad_arrived = fetch_rows(slot_token, grad_all.reshape(rank_count, length, model_width))
    hidden_state_gradient = jnp.einsum(
        "erd,efd->erf", grad_arrived, expert_down, preferred_element_type=jnp.float32
    )
    received_rows = fetch_rows(slot_token, rows_all.reshape(rank_count, length, model_width))
    grad_inputs, expert_hidden, weighted_hidden, expert_gate_gradient, expert_up_gradient = (
        expert_pass(received_rows, hidden_state_gradient, gate_up, slot_weight)
    )

    def cut_back(rows, extra=None):
        other = return_rows(other_order, step_starts, near_token, rows, length)
        arrived = [[swap_cores(piece) for piece in half] for half in other]
        held = return_rows(
            own_order, step_starts, near_token, rows, length, extra, arrived
        )
        return held, other

    grad_cut, grad_other = cut_back(grad_inputs)
    expert_out = jnp.einsum(
        "erf,efd->erd", after(expert_hidden, grad_other[0][0]), expert_down,
        preferred_element_type=jnp.float32,
    )
    expert_out = (expert_out * slot_weight[..., None]).astype(jnp.bfloat16)
    grad_expert_down = jnp.einsum(
        "erf,erd->efd", weighted_hidden, grad_arrived, preferred_element_type=jnp.float32
    )
    grad_expert_gate = jnp.einsum(
        "erd,erf->edf", received_rows, expert_gate_gradient, preferred_element_type=jnp.float32
    )
    grad_expert_up = jnp.einsum(
        "erd,erf->edf", received_rows, expert_up_gradient, preferred_element_type=jnp.float32
    )

    hidden_width = shared_gate.shape[1]
    gate_lift_act = jnp.dot(
        feedforward_normed_input, gate_lift_full, preferred_element_type=jnp.float32
    )
    shared_gate_act, shared_up_act = gate_lift_act[:, :hidden_width], gate_lift_act[:, hidden_width:]
    shared_hidden = (jax.nn.silu(shared_gate_act) * shared_up_act).astype(jnp.bfloat16)
    shared_out = jnp.dot(shared_hidden, lower_full, preferred_element_type=jnp.float32).astype(
        jnp.bfloat16
    )
    out_cut, out_other = cut_back(expert_out, shared_out)
    block_out = scatter_all(out_cut)
    output_share = (middle + block_out).astype(jnp.bfloat16)
    output = gather_tensor(output_share)
    grad_out = quarter(cotangent).astype(jnp.float32)
    grad_shared_hidden = dot_last(cotangent, lower_full)
    grad_sgate, grad_sup = swish_derivative(grad_shared_hidden, shared_gate_act, shared_up_act)
    grad_gate_lift = jnp.concatenate(
        [grad_sgate.astype(jnp.bfloat16), grad_sup.astype(jnp.bfloat16)], axis=1
    )
    grad_lower = dot_first(shared_hidden, cotangent).astype(jnp.bfloat16)
    grad_gate_lift_full = dot_first(feedforward_normed_input, grad_gate_lift).astype(jnp.bfloat16)
    shared_grad = dot_last(grad_gate_lift, gate_lift_full).astype(jnp.bfloat16)
    shared_grad_share = scatter_tensor(shared_grad)
    routed_grad = scatter_all(
        grad_cut,
        hold_first=(out_other[0][0], shared_grad, grad_gate_lift_full),
        hold_second=(out_cut[0][0], grad_lower),
        hold_last=(grad_expert_down,),
    )
    grad_normed_two = shared_grad_share + routed_grad
    grad_gain_two = jnp.sum(grad_normed_two * hat_two, axis=0)
    grad_middle = grad_out + norm_back(grad_normed_two * feedforward_norm_scale, hat_two, inv_two)
    grad_middle_low = gather_tensor(grad_middle.astype(jnp.bfloat16))
    grad_middle_low = after(grad_middle_low, grad_expert_up)
    grad_output_full = dot_first(mixed_heads, grad_middle_low)
    grad_mixed = dot_last(grad_middle_low, output_full)
    grad_mixed = (
        grad_mixed.astype(jnp.bfloat16)
        .reshape(length, head_count, VDIM)
    )
    scores = raw_scores()
    attn_probs = jnp.exp(scores - log_total)
    grad_probs = jnp.einsum("thv,shv->hts", grad_mixed, values, preferred_element_type=jnp.float32)
    grad_values = jnp.einsum(
        "hts,thv->shv",
        attn_probs.astype(jnp.bfloat16),
        grad_mixed,
        preferred_element_type=jnp.float32,
    )
    row_delta = jnp.sum(attn_probs * grad_probs, axis=-1, keepdims=True)
    grad_scores = (attn_probs * (grad_probs - row_delta)).astype(jnp.bfloat16)
    grad_q_nope = (
        jnp.einsum("hts,shd->thd", grad_scores, key_nope, preferred_element_type=jnp.float32)
        * score_scale
    )
    grad_q_rope = (
        jnp.einsum("hts,sr->thr", grad_scores, key_rot, preferred_element_type=jnp.float32)
        * score_scale
    )
    grad_k_nope = (
        jnp.einsum(
            "hts,thd->shd", grad_scores, q_rot[..., :NOPE], preferred_element_type=jnp.float32
        )
        * score_scale
    )
    grad_k_rope = jnp.einsum(
        "hts,thr->sr", grad_scores, q_rot[..., NOPE:], preferred_element_type=jnp.float32
    )
    grad_k_rope = grad_k_rope * score_scale
    grad_queries = jnp.concatenate(
        [grad_q_nope, rotate(grad_q_rope, cosine[:, None, :], -sine_part[:, None, :])], axis=-1
    )
    grad_queries = grad_queries.astype(jnp.bfloat16).reshape(length, head_count * (NOPE + ROPE))
    grad_keyval = (
        jnp.concatenate([grad_k_nope, grad_values], axis=-1)
        .astype(jnp.bfloat16)
        .reshape(length, head_count * (NOPE + VDIM))
    )
    grad_query_full = dot_first(normed_one, grad_queries)
    grad_expand_full = dot_first(latent_low, grad_keyval)
    grad_latent = dot_last(grad_keyval, expand_full)
    grad_gain_kv = jnp.sum(grad_latent * hat_kv, axis=0)
    grad_latent_raw = norm_back(grad_latent * latent_norm_scale, hat_kv, inv_kv)
    grad_compressed = jnp.concatenate(
        [grad_latent_raw, rotate(grad_k_rope, cosine, -sine_part)], axis=-1
    ).astype(jnp.bfloat16)
    grad_latent_full = dot_first(normed_one, grad_compressed).astype(jnp.bfloat16)
    grad_latent_full = grad_latent_full.reshape((rank_count, groups) + kva_weight.shape)
    latent_parts = [pick(grad_latent_full, column, 1)] + [
        shift_tensor(pick(grad_latent_full, (column + j) % groups, 1), j)
        for j in range(1, groups)
    ]
    grad_normed_one = dot_last(grad_queries, query_full) + dot_last(grad_compressed, latent_full)
    grad_normed_one = grad_normed_one.astype(jnp.bfloat16)
    grad_latent_part = total([after(latent_parts[0], grad_normed_one)] + latent_parts[1:])
    grad_normed_one = scatter_tensor(grad_normed_one)
    hat_one_share = quarter(hat_one)
    grad_gain_one = jnp.sum(grad_normed_one * hat_one_share, axis=0)
    grad_tokens = grad_middle + norm_back(
        grad_normed_one * attention_norm_scale, hat_one_share, quarter(inv_one)
    )
    grad_tokens = gather_tensor(grad_tokens.astype(jnp.bfloat16)).astype(jnp.float32)

    grad_gate_lift_share = lax.psum_scatter(
        grad_gate_lift_full, DP, scatter_dimension=0, tiled=True
    ).astype(jnp.float32)
    grad_shared_gate = grad_gate_lift_share[:, :hidden_width]
    grad_shared_up = grad_gate_lift_share[:, hidden_width:]
    grad_shared_down = lax.psum_scatter(
        grad_lower, DP, scatter_dimension=1, tiled=True
    ).astype(jnp.float32)
    grad_out_weight = lax.psum_scatter(
        grad_output_full.astype(jnp.bfloat16), DP, scatter_dimension=1, tiled=True
    ).astype(jnp.float32)
    query_width, expand_width = 4 * q_weight.shape[1], kvb_weight.shape[1]
    packed_rows = grad_expand_full.shape[0]
    packed_grad = jnp.concatenate(
        [
            side_by_side(grad_query_full.astype(jnp.bfloat16), rank_count),
            grad_expand_full.astype(jnp.bfloat16),
            grad_latent_part.astype(jnp.bfloat16).reshape(packed_rows, -1),
        ],
        axis=1,
    )
    packed_share = lax.psum_scatter(packed_grad, DP, scatter_dimension=0, tiled=True)
    grad_q_weight = stacked(packed_share[:, :query_width], 1).astype(jnp.float32)
    grad_kvb_weight = packed_share[:, query_width : query_width + expand_width].astype(jnp.float32)
    grad_kva_weight = packed_share[:, query_width + expand_width :].astype(jnp.float32)
    grad_kva_weight = grad_kva_weight.reshape(kva_weight.shape)
    gain_grads = jnp.concatenate(
        [
            grad.reshape(rank_count, groups, -1)
            for grad in (grad_gain_one, grad_gain_kv, grad_gain_two)
        ],
        axis=2,
    )
    gain_grads = scatter_small(
        gain_grads, (grad_shared_gate, grad_shared_up, grad_shared_down, grad_out_weight)
    )
    grad_norm1_gain = gain_grads[: gain_widths[0]]
    grad_kv_gain = gain_grads[gain_widths[0] : gain_widths[0] + gain_widths[1]]
    grad_norm2_gain = gain_grads[gain_widths[0] + gain_widths[1] :]
    return (
        output,
        grad_tokens,
        grad_norm1_gain,
        grad_q_weight,
        grad_kva_weight,
        grad_kv_gain,
        grad_kvb_weight,
        grad_out_weight,
        grad_norm2_gain,
        grad_shared_gate,
        grad_shared_up,
        grad_shared_down,
        grad_expert_gate,
        grad_expert_up,
        grad_expert_down,
    )


def solution(mesh):
    in_specs = (
        P(DP, None),
        P(DP, None),
        P(DP, None),
        P(DP, None),
        P((DP, TP)),
        P(DP, TP),
        P((DP, TP), None),
        P((DP, TP)),
        P(DP, TP),
        P(TP, DP),
        P((DP, TP)),
        P(DP, TP),
        P(DP, TP),
        P(TP, DP),
        P(DP, None, TP),
        P(DP, None, TP),
        P(DP, TP, None),
        P(DP, None),
    )
    out_specs = (
        P(DP, None),
        P(DP, None),
        P((DP, TP)),
        P(DP, TP),
        P((DP, TP), None),
        P((DP, TP)),
        P(DP, TP),
        P(TP, DP),
        P((DP, TP)),
        P(DP, TP),
        P(DP, TP),
        P(TP, DP),
        P(DP, None, TP),
        P(DP, None, TP),
        P(DP, TP, None),
    )

    return jax.shard_map(local, mesh=mesh, in_specs=in_specs, out_specs=out_specs, check_vma=False)
```

```python
import functools

import jax
import jax.numpy as jnp
from jax import lax
from jax.experimental import pallas as pl
from jax.experimental.pallas import tpu as pltpu
from jax.sharding import PartitionSpec as P


NOPE = 128
ROPE = 64
VDIM = 128
LATENT = 512
SEGS = 2


DP, TP = "dp", "tensor"
epsilon = 1e-06
theta_base = 10000.0


def dot_last(left, right):
    return lax.dot_general(
        left,
        right,
        (((left.ndim - 1,), (right.ndim - 1,)), ((), ())),
        preferred_element_type=jnp.float32,
    )


def dot_first(left, right):
    return lax.dot_general(
        left, right, (((0,), (0,)), ((), ())), preferred_element_type=jnp.float32
    )


def rotate(vector, cosine, sine_part):
    half_width = vector.shape[-1] // 2
    lower_half = vector[..., :half_width]
    upper_half = vector[..., half_width:]
    return jnp.concatenate(
        [
            lower_half * cosine - upper_half * sine_part,
            upper_half * cosine + lower_half * sine_part,
        ],
        axis=-1,
    )


def angles(segment_row):
    seq_len = segment_row.shape[0]
    member = segment_row[:, None] == jnp.arange(SEGS, dtype=jnp.int32)[None, :]
    seq_sizes = jnp.sum(member.astype(jnp.int32), axis=0)
    starts = jnp.cumsum(seq_sizes) - seq_sizes
    seq_first = jnp.sum(jnp.where(member, starts[None, :], 0), axis=1)
    seq_place = (jnp.arange(seq_len, dtype=jnp.int32) - seq_first).astype(jnp.float32)
    inv_freq = theta_base ** (-2.0 * jnp.arange(ROPE // 2, dtype=jnp.float32) / ROPE)
    angle_all = seq_place[:, None] * inv_freq[None, :]
    return (jnp.cos(angle_all), jnp.sin(angle_all))


def norm_scale(vector):
    return lax.rsqrt(jnp.mean(vector * vector, axis=-1, keepdims=True) + epsilon)


def norm_back(grad_hat, hat_value, inv_root):
    return inv_root * (
        grad_hat - hat_value * jnp.mean(grad_hat * hat_value, axis=-1, keepdims=True)
    )


def swish_derivative(grad_act, gate_act, up_act):
    sigma = jax.nn.sigmoid(gate_act)
    return (
        grad_act * up_act * sigma * (1.0 + gate_act * (1.0 - sigma)),
        grad_act * gate_act * sigma,
    )


def after(value, *earlier):
    if not earlier:
        return value
    return lax.optimization_barrier((value,) + earlier)[0]


def shift_tensor(value, step):
    size = lax.axis_size(TP)
    return lax.ppermute(value, TP, [(i, (i + step) % size) for i in range(size)])


def shift_chips(value, step):
    chips = lax.axis_size(DP) // 2
    pairs = [(2 * z + c, 2 * ((z + step) % chips) + c) for z in range(chips) for c in range(2)]
    return lax.ppermute(value, DP, pairs)


def swap_cores(value):
    return lax.ppermute(value, DP, [(i, i ^ 1) for i in range(lax.axis_size(DP))])


def pick(value, index, axis=0):
    return lax.dynamic_index_in_dim(value, index, axis, keepdims=False)


def place(pieces, owners, hold=()):
    whole = after(jnp.zeros((len(pieces),) + pieces[0].shape, pieces[0].dtype), *hold)
    for piece, owner in zip(pieces, owners):
        whole = lax.dynamic_update_index_in_dim(whole, piece, owner, 0)
    return whole


def gather_dp(value, hold=()):
    ranks = lax.axis_size(DP)
    chips = ranks // 2
    index = lax.axis_index(DP)
    core, chip = index % 2, index // 2
    mine = [value] + [shift_chips(value, k) for k in range(1, chips)]
    other = [swap_cores(piece) for piece in mine]
    origin = [(chip - k) % chips for k in range(chips)]
    owners = [2 * z + core for z in origin] + [2 * z + 1 - core for z in origin]
    return place(mine + other, owners, hold)


def gather_tensor(value):
    size = lax.axis_size(TP)
    index = lax.axis_index(TP)
    pieces = [value] + [shift_tensor(value, j) for j in range(1, size)]
    whole = place(pieces, [(index - j) % size for j in range(size)])
    return whole.reshape((size * value.shape[0],) + value.shape[1:])


def total(pieces):
    whole = pieces[0].astype(jnp.float32)
    for piece in pieces[1:]:
        whole = whole + piece.astype(jnp.float32)
    return whole


def scatter_tensor(value):
    size = lax.axis_size(TP)
    index = lax.axis_index(TP)
    value = value.reshape((size, value.shape[0] // size) + value.shape[1:])
    pieces = [shift_tensor(pick(value, (index + j) % size), j) for j in range(1, size)]
    return total([pick(value, index)] + pieces)


def shift_outer(value, step):
    size = lax.axis_size(TP)
    inner = size // 2
    pairs = [(i, (i + step * inner) % size) for i in range(size)]
    return lax.ppermute(value, TP, pairs)


def shift_inner(value, step):
    size = lax.axis_size(TP)
    inner = size // 2
    pairs = [(i, i // inner * inner + (i + step) % inner) for i in range(size)]
    return lax.ppermute(value, TP, pairs)


def scatter_half(held, inner_first, hold_first, hold_second, hold_last):
    inner = len(held) // 2
    chips, dtype = held[0].shape[0], held[0].dtype
    if inner_first:
        groups = [[held[o * inner + i] for i in range(inner)] for o in range(2)]
        first, second = shift_inner, shift_outer
    else:
        groups = [[held[o * inner + i] for o in range(2)] for i in range(inner)]
        first, second = shift_outer, shift_inner
    moved = [[first(group[n], n) for n in range(1, len(group))] for group in groups]
    sums = [
        total([after(group[0], *hold_first)] + arrived).astype(dtype)
        for group, arrived in zip(groups, moved)
    ]
    moved = [second(sums[n], n) for n in range(1, len(sums))]
    kept = after(sums[0], *hold_second)
    pieces = [total([kept[k]] + [piece[k] for piece in moved]).astype(dtype) for k in range(chips)]
    moved = [shift_chips(pieces[k], k) for k in range(1, chips)]
    return total([after(pieces[0], *hold_last)] + moved)


def scatter_all(held, hold_first=(), hold_second=(), hold_last=()):
    return jnp.concatenate(
        [
            scatter_half(half, n == 0, hold_first, hold_second, hold_last)
            for n, half in enumerate(held)
        ],
        axis=1,
    )


def scatter_small(value, hold):
    ranks, size = lax.axis_size(DP), lax.axis_size(TP)
    index, column = lax.axis_index(DP), lax.axis_index(TP)
    core, chip = index % 2, index // 2
    value = value.reshape(ranks // 2, 2, size, value.shape[-1])
    value = pick(value, core, 1) + swap_cores(pick(value, 1 - core, 1))
    pieces = [shift_tensor(pick(value, (column + j) % size, 1), j) for j in range(1, size)]
    value = total([pick(value, column, 1)] + pieces)
    value = after(value, *hold)
    pieces = [shift_chips(pick(value, (chip + k) % (ranks // 2)), k) for k in range(1, ranks // 2)]
    return total([pick(value, chip)] + pieces)


def slot_tables(ids_all, weights_all, first_expert, local_experts, capacity):
    length = ids_all.shape[2]
    experts = first_expert + jnp.arange(local_experts, dtype=jnp.int32)
    named = ids_all[:, None] == experts[None, :, None, None]
    member = jnp.any(named, axis=2)
    pair_weight = jnp.sum(jnp.where(named, weights_all[:, None], 0.0), axis=2)
    earlier = jnp.arange(length)[:, None] < jnp.arange(length)[None, :]
    rank = jnp.einsum(
        "set,tu->seu",
        member.astype(jnp.bfloat16),
        earlier.astype(jnp.bfloat16),
        preferred_element_type=jnp.float32,
    ).astype(jnp.int32)
    slot = jnp.where(member, rank, -1)
    chosen = slot[:, :, None, :] == jnp.arange(capacity, dtype=jnp.int32)[None, None, :, None]
    slot_weight = jnp.sum(jnp.where(chosen, pair_weight[:, :, None, :], 0.0), axis=3)
    slot_token = jnp.sum(
        jnp.where(chosen, jnp.arange(length, dtype=jnp.int32) + 1, 0), axis=3
    ) - 1
    return slot_token, slot_weight


def fetch_kernel(token_ref, rows_ref, out_ref):
    experts, room = out_ref.shape[:2]
    slots, length = token_ref.shape[0], rows_ref.shape[0]
    position = lax.broadcasted_iota(jnp.int32, (slots, length), 1)
    chosen = (token_ref[...] == position).astype(jnp.bfloat16)
    fetched = jnp.dot(chosen, rows_ref[...], preferred_element_type=jnp.float32)
    fetched = fetched.astype(jnp.bfloat16)
    for e in range(experts):
        out_ref[e] = fetched[e * room : (e + 1) * room]


def fetch_rows(slot_token, rows):
    ranks, experts, room = slot_token.shape
    length, width = rows.shape[1:]
    slots = experts * room
    return pl.pallas_call(
        fetch_kernel,
        grid=(ranks,),
        in_specs=[
            pl.BlockSpec((None, slots, 1), lambda s: (s, 0, 0)),
            pl.BlockSpec((None, length, width), lambda s: (s, 0, 0)),
        ],
        out_specs=pl.BlockSpec((experts, room, width), lambda s: (0, s, 0)),
        out_shape=jax.ShapeDtypeStruct((experts, ranks * room, width), jnp.bfloat16),
        cost_estimate=pl.CostEstimate(
            flops=2 * ranks * slots * length * width,
            bytes_accessed=2 * ranks * (slots + length) * width,
            transcendentals=0,
        ),
        name="fetch_rows",
    )(slot_token.reshape(ranks, slots, 1), rows)


def return_kernel(with_extra, order_ref, start_ref, token_ref, rows_ref, *refs):
    experts, room, width = rows_ref.shape
    extra_ref, refs = (refs[0], refs[1:]) if with_extra else (None, refs)
    size, count = start_ref.shape[0], refs[0].shape[0]
    arrived_refs, out_refs = refs[: -2 * size], refs[-2 * size :]
    rows = rows_ref[...].reshape(experts * room, width)
    position = lax.broadcasted_iota(jnp.int32, (count, experts * room), 0)
    for step in range(size):
        chosen = (token_ref[...] == position + step * count).astype(jnp.bfloat16)
        sums = jnp.dot(chosen, rows, preferred_element_type=jnp.float32)
        if with_extra:
            begin = pl.multiple_of(start_ref[step] * count, count)
            extra = extra_ref[pl.ds(begin, count)].astype(jnp.float32)
            sums = sums + jnp.where(pl.program_id(0) == 0, extra, 0.0)
        for half in range(2):
            part = sums[:, half * (width // 2) : (half + 1) * (width // 2)]
            if arrived_refs:
                part = part + arrived_refs[half * size + step][...].astype(jnp.float32)
            out_refs[half * size + step][...] = part.astype(jnp.bfloat16)


def return_rows(order, starts, slot_token, rows, length, extra=None, arrived=None):
    steps, (ranks, experts, room), width = order.shape[0], slot_token.shape, rows.shape[2]
    size, slots = starts.shape[0], experts * room
    count = length // size
    more = [] if extra is None else [extra]
    more_specs = [] if extra is None else [pl.BlockSpec((length, width), lambda k, o, s: (0, 0))]
    cut_specs = [pl.BlockSpec((None, count, width // 2), lambda k, o, s: (k, 0, 0))] * (2 * size)
    if arrived is not None:
        more = more + list(arrived[0]) + list(arrived[1])
        more_specs = more_specs + cut_specs
    results = pl.pallas_call(
        functools.partial(return_kernel, extra is not None),
        grid_spec=pltpu.PrefetchScalarGridSpec(
            num_scalar_prefetch=2,
            grid=(steps,),
            in_specs=[
                pl.BlockSpec((None, 1, slots), lambda k, o, s: (o[k], 0, 0)),
                pl.BlockSpec((experts, room, width), lambda k, o, s: (0, o[k], 0)),
            ]
            + more_specs,
            out_specs=cut_specs,
        ),
        out_shape=[jax.ShapeDtypeStruct((steps, count, width // 2), jnp.bfloat16)] * (2 * size),
        cost_estimate=pl.CostEstimate(
            flops=2 * steps * slots * length * width,
            bytes_accessed=2 * steps * (slots + 2 * length) * width,
            transcendentals=0,
        ),
        name="return_rows",
    )(order, starts, slot_token.reshape(ranks, 1, slots), rows, *more)
    return results[:size], results[size:]


def expert_kernel(
    rows_ref, grad_ref, weight_ref, slot_ref, back_ref, hidden_ref, scaled_ref, gate_ref, up_ref, both
):
    width = grad_ref.shape[1]
    half = weight_ref.shape[1] // 2

    @pl.when((pl.program_id(0) == 0) & (pl.program_id(1) == 0))
    def _():
        both[...] = jnp.zeros_like(both)

    acts = jnp.dot(rows_ref[...], weight_ref[...], preferred_element_type=jnp.float32)
    gate_act, up_act = acts[:, :width], acts[:, half : half + width]
    sigma = 1.0 / (1.0 + jnp.exp(-gate_act))
    silu = gate_act * sigma
    hidden = (silu * up_act).astype(jnp.bfloat16)
    hidden_ref[...] = hidden
    scaled_ref[...] = (hidden.astype(jnp.float32) * slot_ref[...]).astype(jnp.bfloat16)
    grad = grad_ref[...] * slot_ref[...]
    gate_grad = (grad * up_act * sigma * (1.0 + gate_act * (1.0 - sigma))).astype(jnp.bfloat16)
    up_grad = (grad * silu).astype(jnp.bfloat16)
    gate_ref[...] = gate_grad
    up_ref[...] = up_grad
    both[:, :width] = gate_grad
    both[:, half : half + width] = up_grad
    back_ref[...] = lax.dot_general(
        both[...], weight_ref[...], (((1,), (1,)), ((), ())), preferred_element_type=jnp.float32
    ).astype(jnp.bfloat16)


def expert_pass(rows, grad_hidden, weights, slot_weight):
    experts, slots, width = rows.shape
    hidden = grad_hidden.shape[2]
    share = slots // 2
    row_spec = pl.BlockSpec((None, share, width), lambda e, i: (e, i, 0))
    hidden_spec = pl.BlockSpec((None, share, hidden), lambda e, i: (e, i, 0))
    hidden_shape = jax.ShapeDtypeStruct((experts, slots, hidden), jnp.bfloat16)
    return pl.pallas_call(
        expert_kernel,
        grid=(experts, 2),
        in_specs=[
            row_spec,
            hidden_spec,
            pl.BlockSpec((None,) + weights.shape[1:], lambda e, i: (e, 0, 0)),
            pl.BlockSpec((None, share, 1), lambda e, i: (e, i, 0)),
        ],
        out_specs=[row_spec] + [hidden_spec] * 4,
        out_shape=[jax.ShapeDtypeStruct(rows.shape, jnp.bfloat16)] + [hidden_shape] * 4,
        scratch_shapes=[pltpu.VMEM((share, weights.shape[2]), jnp.bfloat16)],
        cost_estimate=pl.CostEstimate(
            flops=8 * experts * slots * width * hidden,
            bytes_accessed=4 * experts * (slots + hidden) * width,
            transcendentals=experts * slots * hidden,
        ),
        name="expert_pass",
    )(rows, grad_hidden, weights, slot_weight[..., None])


def side_by_side(value, ranks):
    width = value.shape[1]
    value = value.reshape(ranks, 4, -1, width).transpose(0, 2, 1, 3)
    return value.reshape(-1, 4 * width)


def stacked(value, ranks):
    width = value.shape[1] // 4
    value = value.reshape(ranks, -1, 4, width).transpose(0, 2, 1, 3)
    return value.reshape(-1, width)


def local(
    tokens,
    segments,
    expert_ids,
    route_weight,
    norm1_gain,
    q_weight,
    kva_weight,
    kv_gain,
    kvb_weight,
    out_weight,
    norm2_gain,
    shared_gate,
    shared_up,
    shared_down,
    expert_gate,
    expert_up_projection,
    expert_down,
    cotangent,
):
    length = tokens.shape[0]
    model_width = tokens.shape[1]
    groups = lax.axis_size(TP)
    rank_count = lax.axis_size(DP)
    local_experts = expert_gate.shape[0]
    experts_all = local_experts * rank_count
    choose = expert_ids.shape[1]
    capacity = groups * -(-(3 * length * choose) // (2 * experts_all * groups))
    slot_room = 16 * -(-capacity // 16)
    head_count = q_weight.shape[1] // (NOPE + ROPE)
    score_scale = (NOPE + ROPE) ** (-0.5)
    dp_index = lax.axis_index(DP)
    column = lax.axis_index(TP)
    chips = rank_count // 2
    token_share = length // groups

    def quarter(rows):
        return lax.dynamic_slice_in_dim(rows, column * token_share, token_share, 0)

    gain_widths = (norm1_gain.shape[0], kv_gain.shape[0], norm2_gain.shape[0])
    latent_rows, latent_width = kva_weight.shape
    gain_row = jnp.concatenate([norm1_gain, kv_gain, norm2_gain])
    gain_columns = -(-sum(gain_widths) // latent_rows)
    gain_row = jnp.pad(gain_row, (0, gain_columns * latent_rows - sum(gain_widths)))
    small = jnp.concatenate([kva_weight, gain_row.reshape(latent_rows, gain_columns)], axis=1)
    small = gather_dp(small)
    pieces = [small] + [shift_tensor(small, j) for j in range(1, groups)]
    pieces = tuple(pieces)
    small_all = jnp.zeros((rank_count, groups) + small.shape[1:], small.dtype)
    for j, piece in enumerate(pieces):
        small_all = lax.dynamic_update_index_in_dim(small_all, piece, (column - j) % groups, 1)
    small_all = small_all.reshape(-1, latent_width + gain_columns)
    latent_full = small_all[:, :latent_width]
    gains_all = small_all[:, latent_width:].reshape(rank_count * groups, -1).astype(jnp.float32)
    attention_norm_scale = gains_all[:, : gain_widths[0]].reshape(-1)
    latent_norm_scale = gains_all[:, gain_widths[0] : gain_widths[0] + gain_widths[1]].reshape(-1)
    feedforward_norm_scale = gains_all[:, gain_widths[0] + gain_widths[1] : sum(gain_widths)].reshape(-1)

    expand_full = gather_dp(kvb_weight, pieces).reshape(-1, kvb_weight.shape[1])
    query_full = gather_dp(q_weight, pieces).reshape(-1, q_weight.shape[1])
    output_rows = gather_dp(after(out_weight, small_all))
    output_full = output_rows.transpose(1, 0, 2).reshape(out_weight.shape[0], -1)

    routing = jnp.concatenate([expert_ids.astype(jnp.float32).T, route_weight.T], axis=0)
    routing_all = gather_dp(routing)
    ids_all, weights_all = routing_all[:, :choose].astype(jnp.int32), routing_all[:, choose:]
    grad_all = lax.all_gather(
        after(quarter(cotangent), small), (DP, TP), axis=0, tiled=True
    )
    residual_stream = tokens.astype(jnp.float32)
    inv_one = norm_scale(residual_stream)
    hat_one = residual_stream * inv_one
    normed_one = (hat_one * attention_norm_scale).astype(jnp.bfloat16)
    segment_row = segments[0]
    cosine, sine_part = angles(segment_row)
    queries = jnp.dot(normed_one, query_full, preferred_element_type=jnp.float32).reshape(
        length, head_count, NOPE + ROPE
    )
    q_rot = jnp.concatenate(
        [
            queries[..., :NOPE],
            rotate(queries[..., NOPE:], cosine[:, None, :], sine_part[:, None, :]),
        ],
        axis=-1,
    ).astype(jnp.bfloat16)
    compressed = jnp.dot(normed_one, latent_full, preferred_element_type=jnp.float32)
    latent_raw = compressed[:, :LATENT]
    inv_kv = norm_scale(latent_raw)
    hat_kv = latent_raw * inv_kv
    latent_low = (hat_kv * latent_norm_scale).astype(jnp.bfloat16)
    key_rot = rotate(compressed[:, LATENT:], cosine, sine_part).astype(jnp.bfloat16)
    keyval = (
        jnp.dot(latent_low, expand_full, preferred_element_type=jnp.float32)
        .astype(jnp.bfloat16)
        .reshape(length, head_count, NOPE + VDIM)
    )
    key_nope = keyval[..., :NOPE]
    values = keyval[..., NOPE:]
    positions = jnp.arange(length, dtype=jnp.int32)
    allowed = (segment_row[:, None] == segment_row[None, :]) & (
        positions[None, :] <= positions[:, None]
    )

    def raw_scores():
        dots = jnp.einsum(
            "thd,shd->hts", q_rot[..., :NOPE], key_nope, preferred_element_type=jnp.float32
        )
        dots = dots + jnp.einsum(
            "thr,sr->hts", q_rot[..., NOPE:], key_rot, preferred_element_type=jnp.float32
        )
        return jnp.where(allowed[None], dots * score_scale, -1000000000.0)

    scores = raw_scores()
    row_peak = jnp.max(scores, axis=-1, keepdims=True)
    log_total = jnp.log(jnp.sum(jnp.exp(scores - row_peak), axis=-1, keepdims=True)) + row_peak
    attn_probs = jnp.exp(scores - log_total)
    mixed_heads = (
        jnp.einsum(
            "hts,shv->thv",
            attn_probs.astype(jnp.bfloat16),
            values,
            preferred_element_type=jnp.float32,
        )
        .astype(jnp.bfloat16)
        .reshape(length, head_count * VDIM)
    )
    attn_out = scatter_tensor(
        jnp.dot(mixed_heads, output_full, preferred_element_type=jnp.float32).astype(jnp.bfloat16)
    )
    middle = quarter(tokens).astype(jnp.float32) + after(attn_out, grad_all)
    inv_two = norm_scale(middle)
    hat_two = middle * inv_two
    normed_two = (hat_two * feedforward_norm_scale).astype(jnp.bfloat16)
    rows_all = lax.all_gather(normed_two, (DP, TP), axis=0, tiled=True)
    feedforward_normed_input = lax.dynamic_slice_in_dim(rows_all, dp_index * length, length, 0)

    gate_lift_full = lax.all_gather(
        jnp.concatenate([shared_gate, shared_up], axis=1), DP, axis=0, tiled=True
    )
    lower_full = lax.all_gather(shared_down, DP, axis=1, tiled=True)

    slot_token, slot_weight = slot_tables(
        ids_all, weights_all, dp_index * local_experts, local_experts, slot_room
    )
    inner = groups // 2
    share = slot_token // token_share
    step = (share // inner - column // inner) % 2 * inner + (share - column) % inner
    outer_steps = jnp.arange(groups, dtype=jnp.int32) // inner
    inner_steps = jnp.arange(groups, dtype=jnp.int32) % inner
    step_starts = (column // inner + outer_steps) % 2 * inner + (column + inner_steps) % inner
    near_token = jnp.where(slot_token < 0, -1, step * token_share + slot_token % token_share)
    slot_weight = slot_weight.transpose(1, 0, 2).reshape(local_experts, -1)
    chip_steps = (dp_index // 2 + jnp.arange(chips, dtype=jnp.int32)) % chips
    own_order = 2 * chip_steps + dp_index % 2
    other_order = 2 * chip_steps + 1 - dp_index % 2
    expert_width = expert_gate.shape[2]
    lane_pad = ((0, 0), (0, 0), (0, -expert_width % 128))
    gate_up = jnp.concatenate(
        [jnp.pad(expert_gate, lane_pad), jnp.pad(expert_up_projection, lane_pad)], axis=2
    )
    grad_arrived = fetch_rows(slot_token, grad_all.reshape(rank_count, length, model_width))
    hidden_state_gradient = jnp.einsum(
        "erd,efd->erf", grad_arrived, expert_down, preferred_element_type=jnp.float32
    )
    received_rows = fetch_rows(slot_token, rows_all.reshape(rank_count, length, model_width))
    grad_inputs, expert_hidden, weighted_hidden, expert_gate_gradient, expert_up_gradient = (
        expert_pass(received_rows, hidden_state_gradient, gate_up, slot_weight)
    )

    def cut_back(rows, extra=None):
        other = return_rows(other_order, step_starts, near_token, rows, length)
        arrived = [[swap_cores(piece) for piece in half] for half in other]
        held = return_rows(
            own_order, step_starts, near_token, rows, length, extra, arrived
        )
        return held, other

    grad_cut, grad_other = cut_back(grad_inputs)
    expert_out = jnp.einsum(
        "erf,efd->erd", after(expert_hidden, grad_other[0][0]), expert_down,
        preferred_element_type=jnp.float32,
    )
    expert_out = (expert_out * slot_weight[..., None]).astype(jnp.bfloat16)
    grad_expert_down = jnp.einsum(
        "erf,erd->efd", weighted_hidden, grad_arrived, preferred_element_type=jnp.float32
    )
    grad_expert_gate = jnp.einsum(
        "erd,erf->edf", received_rows, expert_gate_gradient, preferred_element_type=jnp.float32
    )
    grad_expert_up = jnp.einsum(
        "erd,erf->edf", received_rows, expert_up_gradient, preferred_element_type=jnp.float32
    )

    hidden_width = shared_gate.shape[1]
    gate_lift_act = jnp.dot(
        feedforward_normed_input, gate_lift_full, preferred_element_type=jnp.float32
    )
    shared_gate_act, shared_up_act = gate_lift_act[:, :hidden_width], gate_lift_act[:, hidden_width:]
    shared_hidden = (jax.nn.silu(shared_gate_act) * shared_up_act).astype(jnp.bfloat16)
    shared_out = jnp.dot(shared_hidden, lower_full, preferred_element_type=jnp.float32).astype(
        jnp.bfloat16
    )
    out_cut, out_other = cut_back(expert_out, shared_out)
    block_out = scatter_all(out_cut)
    output_share = (middle + block_out).astype(jnp.bfloat16)
    output = gather_tensor(output_share)
    grad_out = quarter(cotangent).astype(jnp.float32)
    grad_shared_hidden = dot_last(cotangent, lower_full)
    grad_sgate, grad_sup = swish_derivative(grad_shared_hidden, shared_gate_act, shared_up_act)
    grad_gate_lift = jnp.concatenate(
        [grad_sgate.astype(jnp.bfloat16), grad_sup.astype(jnp.bfloat16)], axis=1
    )
    grad_lower = dot_first(shared_hidden, cotangent).astype(jnp.bfloat16)
    grad_gate_lift_full = dot_first(feedforward_normed_input, grad_gate_lift).astype(jnp.bfloat16)
    shared_grad = dot_last(grad_gate_lift, gate_lift_full).astype(jnp.bfloat16)
    shared_grad_share = scatter_tensor(shared_grad)
    routed_grad = scatter_all(
        grad_cut,
        hold_first=(out_other[0][0], shared_grad, grad_gate_lift_full),
        hold_second=(out_cut[0][0], grad_lower),
        hold_last=(grad_expert_down, grad_expert_gate, grad_expert_up),
    )
    grad_normed_two = shared_grad_share + routed_grad
    grad_gain_two = jnp.sum(grad_normed_two * hat_two, axis=0)
    grad_middle = grad_out + norm_back(grad_normed_two * feedforward_norm_scale, hat_two, inv_two)
    grad_middle_low = gather_tensor(grad_middle.astype(jnp.bfloat16))
    grad_output_full = dot_first(mixed_heads, grad_middle_low)
    grad_mixed = dot_last(grad_middle_low, output_full)
    grad_mixed = (
        grad_mixed.astype(jnp.bfloat16)
        .reshape(length, head_count, VDIM)
    )
    scores = raw_scores()
    attn_probs = jnp.exp(scores - log_total)
    grad_probs = jnp.einsum("thv,shv->hts", grad_mixed, values, preferred_element_type=jnp.float32)
    grad_values = jnp.einsum(
        "hts,thv->shv",
        attn_probs.astype(jnp.bfloat16),
        grad_mixed,
        preferred_element_type=jnp.float32,
    )
    row_delta = jnp.sum(attn_probs * grad_probs, axis=-1, keepdims=True)
    grad_scores = (attn_probs * (grad_probs - row_delta)).astype(jnp.bfloat16)
    grad_q_nope = (
        jnp.einsum("hts,shd->thd", grad_scores, key_nope, preferred_element_type=jnp.float32)
        * score_scale
    )
    grad_q_rope = (
        jnp.einsum("hts,sr->thr", grad_scores, key_rot, preferred_element_type=jnp.float32)
        * score_scale
    )
    grad_k_nope = (
        jnp.einsum(
            "hts,thd->shd", grad_scores, q_rot[..., :NOPE], preferred_element_type=jnp.float32
        )
        * score_scale
    )
    grad_k_rope = jnp.einsum(
        "hts,thr->sr", grad_scores, q_rot[..., NOPE:], preferred_element_type=jnp.float32
    )
    grad_k_rope = grad_k_rope * score_scale
    grad_queries = jnp.concatenate(
        [grad_q_nope, rotate(grad_q_rope, cosine[:, None, :], -sine_part[:, None, :])], axis=-1
    )
    grad_queries = grad_queries.astype(jnp.bfloat16).reshape(length, head_count * (NOPE + ROPE))
    grad_keyval = (
        jnp.concatenate([grad_k_nope, grad_values], axis=-1)
        .astype(jnp.bfloat16)
        .reshape(length, head_count * (NOPE + VDIM))
    )
    grad_query_full = dot_first(normed_one, grad_queries)
    grad_expand_full = dot_first(latent_low, grad_keyval)
    grad_latent = dot_last(grad_keyval, expand_full)
    grad_gain_kv = jnp.sum(grad_latent * hat_kv, axis=0)
    grad_latent_raw = norm_back(grad_latent * latent_norm_scale, hat_kv, inv_kv)
    grad_compressed = jnp.concatenate(
        [grad_latent_raw, rotate(grad_k_rope, cosine, -sine_part)], axis=-1
    ).astype(jnp.bfloat16)
    grad_latent_full = dot_first(normed_one, grad_compressed).astype(jnp.bfloat16)
    grad_latent_full = grad_latent_full.reshape((rank_count, groups) + kva_weight.shape)
    latent_parts = [pick(grad_latent_full, column, 1)] + [
        shift_tensor(pick(grad_latent_full, (column + j) % groups, 1), j)
        for j in range(1, groups)
    ]
    grad_normed_one = dot_last(grad_queries, query_full)
    grad_normed_one = grad_normed_one + dot_last(grad_compressed, latent_full)
    grad_normed_one = grad_normed_one.astype(jnp.bfloat16)
    grad_latent_part = total([after(latent_parts[0], grad_normed_one)] + latent_parts[1:])
    grad_normed_one = scatter_tensor(grad_normed_one)
    hat_one_share = quarter(hat_one)
    grad_gain_one = jnp.sum(grad_normed_one * hat_one_share, axis=0)
    grad_tokens = grad_middle + norm_back(
        grad_normed_one * attention_norm_scale, hat_one_share, quarter(inv_one)
    )
    grad_tokens = gather_tensor(grad_tokens.astype(jnp.bfloat16)).astype(jnp.float32)

    grad_gate_lift_share = lax.psum_scatter(
        grad_gate_lift_full, DP, scatter_dimension=0, tiled=True
    ).astype(jnp.float32)
    grad_shared_gate = grad_gate_lift_share[:, :hidden_width]
    grad_shared_up = grad_gate_lift_share[:, hidden_width:]
    grad_shared_down = lax.psum_scatter(
        grad_lower, DP, scatter_dimension=1, tiled=True
    ).astype(jnp.float32)
    grad_out_weight = lax.psum_scatter(
        grad_output_full.astype(jnp.bfloat16), DP, scatter_dimension=1, tiled=True
    ).astype(jnp.float32)
    query_width, expand_width = 4 * q_weight.shape[1], kvb_weight.shape[1]
    packed_rows = grad_expand_full.shape[0]
    packed_grad = jnp.concatenate(
        [
            side_by_side(grad_query_full.astype(jnp.bfloat16), rank_count),
            grad_expand_full.astype(jnp.bfloat16),
            grad_latent_part.astype(jnp.bfloat16).reshape(packed_rows, -1),
        ],
        axis=1,
    )
    packed_share = lax.psum_scatter(packed_grad, DP, scatter_dimension=0, tiled=True)
    grad_q_weight = stacked(packed_share[:, :query_width], 1).astype(jnp.float32)
    grad_kvb_weight = packed_share[:, query_width : query_width + expand_width].astype(jnp.float32)
    grad_kva_weight = packed_share[:, query_width + expand_width :].astype(jnp.float32)
    grad_kva_weight = grad_kva_weight.reshape(kva_weight.shape)
    gain_grads = jnp.concatenate(
        [
            grad.reshape(rank_count, groups, -1)
            for grad in (grad_gain_one, grad_gain_kv, grad_gain_two)
        ],
        axis=2,
    )
    gain_grads = scatter_small(
        gain_grads, (grad_shared_gate, grad_shared_up, grad_shared_down, grad_out_weight)
    )
    grad_norm1_gain = gain_grads[: gain_widths[0]]
    grad_kv_gain = gain_grads[gain_widths[0] : gain_widths[0] + gain_widths[1]]
    grad_norm2_gain = gain_grads[gain_widths[0] + gain_widths[1] :]
    return (
        output,
        grad_tokens,
        grad_norm1_gain,
        grad_q_weight,
        grad_kva_weight,
        grad_kv_gain,
        grad_kvb_weight,
        grad_out_weight,
        grad_norm2_gain,
        grad_shared_gate,
        grad_shared_up,
        grad_shared_down,
        grad_expert_gate,
        grad_expert_up,
        grad_expert_down,
    )


def solution(mesh):
    in_specs = (
        P(DP, None),
        P(DP, None),
        P(DP, None),
        P(DP, None),
        P((DP, TP)),
        P(DP, TP),
        P((DP, TP), None),
        P((DP, TP)),
        P(DP, TP),
        P(TP, DP),
        P((DP, TP)),
        P(DP, TP),
        P(DP, TP),
        P(TP, DP),
        P(DP, None, TP),
        P(DP, None, TP),
        P(DP, TP, None),
        P(DP, None),
    )
    out_specs = (
        P(DP, None),
        P(DP, None),
        P((DP, TP)),
        P(DP, TP),
        P((DP, TP), None),
        P((DP, TP)),
        P(DP, TP),
        P(TP, DP),
        P((DP, TP)),
        P(DP, TP),
        P(DP, TP),
        P(TP, DP),
        P(DP, None, TP),
        P(DP, None, TP),
        P(DP, TP, None),
    )

    return jax.shard_map(local, mesh=mesh, in_specs=in_specs, out_specs=out_specs, check_vma=False)
```

```python
import functools

import jax
import jax.numpy as jnp
from jax import lax
from jax.experimental import pallas as pl
from jax.experimental.pallas import tpu as pltpu
from jax.sharding import PartitionSpec as P


NOPE = 128
ROPE = 64
VDIM = 128
LATENT = 512
SEGS = 2


DP, TP = "dp", "tensor"
epsilon = 1e-06
theta_base = 10000.0


def dot_last(left, right):
    return lax.dot_general(
        left,
        right,
        (((left.ndim - 1,), (right.ndim - 1,)), ((), ())),
        preferred_element_type=jnp.float32,
    )


def dot_first(left, right):
    return lax.dot_general(
        left, right, (((0,), (0,)), ((), ())), preferred_element_type=jnp.float32
    )


def rotate(vector, cosine, sine_part):
    half_width = vector.shape[-1] // 2
    lower_half = vector[..., :half_width]
    upper_half = vector[..., half_width:]
    return jnp.concatenate(
        [
            lower_half * cosine - upper_half * sine_part,
            upper_half * cosine + lower_half * sine_part,
        ],
        axis=-1,
    )


def angles(segment_row):
    seq_len = segment_row.shape[0]
    member = segment_row[:, None] == jnp.arange(SEGS, dtype=jnp.int32)[None, :]
    seq_sizes = jnp.sum(member.astype(jnp.int32), axis=0)
    starts = jnp.cumsum(seq_sizes) - seq_sizes
    seq_first = jnp.sum(jnp.where(member, starts[None, :], 0), axis=1)
    seq_place = (jnp.arange(seq_len, dtype=jnp.int32) - seq_first).astype(jnp.float32)
    inv_freq = theta_base ** (-2.0 * jnp.arange(ROPE // 2, dtype=jnp.float32) / ROPE)
    angle_all = seq_place[:, None] * inv_freq[None, :]
    return (jnp.cos(angle_all), jnp.sin(angle_all))


def norm_scale(vector):
    return lax.rsqrt(jnp.mean(vector * vector, axis=-1, keepdims=True) + epsilon)


def norm_back(grad_hat, hat_value, inv_root):
    return inv_root * (
        grad_hat - hat_value * jnp.mean(grad_hat * hat_value, axis=-1, keepdims=True)
    )


def swish_derivative(grad_act, gate_act, up_act):
    sigma = jax.nn.sigmoid(gate_act)
    return (
        grad_act * up_act * sigma * (1.0 + gate_act * (1.0 - sigma)),
        grad_act * gate_act * sigma,
    )


def after(value, *earlier):
    if not earlier:
        return value
    return lax.optimization_barrier((value,) + earlier)[0]


def shift_tensor(value, step):
    size = lax.axis_size(TP)
    return lax.ppermute(value, TP, [(i, (i + step) % size) for i in range(size)])


def shift_chips(value, step):
    chips = lax.axis_size(DP) // 2
    pairs = [(2 * z + c, 2 * ((z + step) % chips) + c) for z in range(chips) for c in range(2)]
    return lax.ppermute(value, DP, pairs)


def swap_cores(value):
    return lax.ppermute(value, DP, [(i, i ^ 1) for i in range(lax.axis_size(DP))])


def pick(value, index, axis=0):
    return lax.dynamic_index_in_dim(value, index, axis, keepdims=False)


def place(pieces, owners, hold=()):
    whole = after(jnp.zeros((len(pieces),) + pieces[0].shape, pieces[0].dtype), *hold)
    for piece, owner in zip(pieces, owners):
        whole = lax.dynamic_update_index_in_dim(whole, piece, owner, 0)
    return whole


def gather_dp(value, hold=()):
    ranks = lax.axis_size(DP)
    chips = ranks // 2
    index = lax.axis_index(DP)
    core, chip = index % 2, index // 2
    mine = [value] + [shift_chips(value, k) for k in range(1, chips)]
    other = [swap_cores(piece) for piece in mine]
    origin = [(chip - k) % chips for k in range(chips)]
    owners = [2 * z + core for z in origin] + [2 * z + 1 - core for z in origin]
    return place(mine + other, owners, hold)


def gather_tensor(value):
    size = lax.axis_size(TP)
    index = lax.axis_index(TP)
    pieces = [value] + [shift_tensor(value, j) for j in range(1, size)]
    whole = place(pieces, [(index - j) % size for j in range(size)])
    return whole.reshape((size * value.shape[0],) + value.shape[1:])


def total(pieces):
    whole = pieces[0].astype(jnp.float32)
    for piece in pieces[1:]:
        whole = whole + piece.astype(jnp.float32)
    return whole


def scatter_tensor(value):
    size = lax.axis_size(TP)
    index = lax.axis_index(TP)
    value = value.reshape((size, value.shape[0] // size) + value.shape[1:])
    pieces = [shift_tensor(pick(value, (index + j) % size), j) for j in range(1, size)]
    return total([pick(value, index)] + pieces)


def shift_outer(value, step):
    size = lax.axis_size(TP)
    inner = size // 2
    pairs = [(i, (i + step * inner) % size) for i in range(size)]
    return lax.ppermute(value, TP, pairs)


def shift_inner(value, step):
    size = lax.axis_size(TP)
    inner = size // 2
    pairs = [(i, i // inner * inner + (i + step) % inner) for i in range(size)]
    return lax.ppermute(value, TP, pairs)


def scatter_half(held, inner_first, hold_first, hold_second, hold_last):
    inner = len(held) // 2
    chips, dtype = held[0].shape[0], held[0].dtype
    if inner_first:
        groups = [[held[o * inner + i] for i in range(inner)] for o in range(2)]
        first, second = shift_inner, shift_outer
    else:
        groups = [[held[o * inner + i] for o in range(2)] for i in range(inner)]
        first, second = shift_outer, shift_inner
    moved = [[first(group[n], n) for n in range(1, len(group))] for group in groups]
    sums = [
        total([after(group[0], *hold_first)] + arrived).astype(dtype)
        for group, arrived in zip(groups, moved)
    ]
    moved = [second(sums[n], n) for n in range(1, len(sums))]
    kept = after(sums[0], *hold_second)
    pieces = [total([kept[k]] + [piece[k] for piece in moved]).astype(dtype) for k in range(chips)]
    moved = [shift_chips(pieces[k], k) for k in range(1, chips)]
    return total([after(pieces[0], *hold_last)] + moved)


def scatter_all(held, hold_first=(), hold_second=(), hold_last=()):
    return jnp.concatenate(
        [
            scatter_half(half, n == 0, hold_first, hold_second, hold_last)
            for n, half in enumerate(held)
        ],
        axis=1,
    )


def scatter_small(value, hold):
    ranks, size = lax.axis_size(DP), lax.axis_size(TP)
    index, column = lax.axis_index(DP), lax.axis_index(TP)
    core, chip = index % 2, index // 2
    value = value.reshape(ranks // 2, 2, size, value.shape[-1])
    value = pick(value, core, 1) + swap_cores(pick(value, 1 - core, 1))
    pieces = [shift_tensor(pick(value, (column + j) % size, 1), j) for j in range(1, size)]
    value = total([pick(value, column, 1)] + pieces)
    value = after(value, *hold)
    pieces = [shift_chips(pick(value, (chip + k) % (ranks // 2)), k) for k in range(1, ranks // 2)]
    return total([pick(value, chip)] + pieces)


def slot_tables(ids_all, weights_all, first_expert, local_experts, capacity):
    length = ids_all.shape[2]
    experts = first_expert + jnp.arange(local_experts, dtype=jnp.int32)
    named = ids_all[:, None] == experts[None, :, None, None]
    member = jnp.any(named, axis=2)
    pair_weight = jnp.sum(jnp.where(named, weights_all[:, None], 0.0), axis=2)
    earlier = jnp.arange(length)[:, None] < jnp.arange(length)[None, :]
    rank = jnp.einsum(
        "set,tu->seu",
        member.astype(jnp.bfloat16),
        earlier.astype(jnp.bfloat16),
        preferred_element_type=jnp.float32,
    ).astype(jnp.int32)
    slot = jnp.where(member, rank, -1)
    chosen = slot[:, :, None, :] == jnp.arange(capacity, dtype=jnp.int32)[None, None, :, None]
    slot_weight = jnp.sum(jnp.where(chosen, pair_weight[:, :, None, :], 0.0), axis=3)
    slot_token = jnp.sum(
        jnp.where(chosen, jnp.arange(length, dtype=jnp.int32) + 1, 0), axis=3
    ) - 1
    return slot_token, slot_weight


def fetch_kernel(token_ref, rows_ref, out_ref):
    experts, room = out_ref.shape[:2]
    slots, length = token_ref.shape[0], rows_ref.shape[0]
    position = lax.broadcasted_iota(jnp.int32, (slots, length), 1)
    chosen = (token_ref[...] == position).astype(jnp.bfloat16)
    fetched = jnp.dot(chosen, rows_ref[...], preferred_element_type=jnp.float32)
    fetched = fetched.astype(jnp.bfloat16)
    for e in range(experts):
        out_ref[e] = fetched[e * room : (e + 1) * room]


def fetch_rows(slot_token, rows):
    ranks, experts, room = slot_token.shape
    length, width = rows.shape[1:]
    slots = experts * room
    return pl.pallas_call(
        fetch_kernel,
        grid=(ranks,),
        in_specs=[
            pl.BlockSpec((None, slots, 1), lambda s: (s, 0, 0)),
            pl.BlockSpec((None, length, width), lambda s: (s, 0, 0)),
        ],
        out_specs=pl.BlockSpec((experts, room, width), lambda s: (0, s, 0)),
        out_shape=jax.ShapeDtypeStruct((experts, ranks * room, width), jnp.bfloat16),
        cost_estimate=pl.CostEstimate(
            flops=2 * ranks * slots * length * width,
            bytes_accessed=2 * ranks * (slots + length) * width,
            transcendentals=0,
        ),
        name="fetch_rows",
    )(slot_token.reshape(ranks, slots, 1), rows)


def return_kernel(with_extra, order_ref, start_ref, token_ref, rows_ref, *refs):
    experts, room, width = rows_ref.shape
    extra_ref, refs = (refs[0], refs[1:]) if with_extra else (None, refs)
    size, count = start_ref.shape[0], refs[0].shape[0]
    arrived_refs, out_refs = refs[: -2 * size], refs[-2 * size :]
    rows = rows_ref[...].reshape(experts * room, width)
    position = lax.broadcasted_iota(jnp.int32, (count, experts * room), 0)
    for step in range(size):
        chosen = (token_ref[...] == position + step * count).astype(jnp.bfloat16)
        sums = jnp.dot(chosen, rows, preferred_element_type=jnp.float32)
        if with_extra:
            begin = pl.multiple_of(start_ref[step] * count, count)
            extra = extra_ref[pl.ds(begin, count)].astype(jnp.float32)
            sums = sums + jnp.where(pl.program_id(0) == 0, extra, 0.0)
        for half in range(2):
            part = sums[:, half * (width // 2) : (half + 1) * (width // 2)]
            if arrived_refs:
                part = part + arrived_refs[half * size + step][...].astype(jnp.float32)
            out_refs[half * size + step][...] = part.astype(jnp.bfloat16)


def return_rows(order, starts, slot_token, rows, length, extra=None, arrived=None):
    steps, (ranks, experts, room), width = order.shape[0], slot_token.shape, rows.shape[2]
    size, slots = starts.shape[0], experts * room
    count = length // size
    more = [] if extra is None else [extra]
    more_specs = [] if extra is None else [pl.BlockSpec((length, width), lambda k, o, s: (0, 0))]
    cut_specs = [pl.BlockSpec((None, count, width // 2), lambda k, o, s: (k, 0, 0))] * (2 * size)
    if arrived is not None:
        more = more + list(arrived[0]) + list(arrived[1])
        more_specs = more_specs + cut_specs
    results = pl.pallas_call(
        functools.partial(return_kernel, extra is not None),
        grid_spec=pltpu.PrefetchScalarGridSpec(
            num_scalar_prefetch=2,
            grid=(steps,),
            in_specs=[
                pl.BlockSpec((None, 1, slots), lambda k, o, s: (o[k], 0, 0)),
                pl.BlockSpec((experts, room, width), lambda k, o, s: (0, o[k], 0)),
            ]
            + more_specs,
            out_specs=cut_specs,
        ),
        out_shape=[jax.ShapeDtypeStruct((steps, count, width // 2), jnp.bfloat16)] * (2 * size),
        cost_estimate=pl.CostEstimate(
            flops=2 * steps * slots * length * width,
            bytes_accessed=2 * steps * (slots + 2 * length) * width,
            transcendentals=0,
        ),
        name="return_rows",
    )(order, starts, slot_token.reshape(ranks, 1, slots), rows, *more)
    return results[:size], results[size:]


def expert_kernel(
    rows_ref, grad_ref, weight_ref, slot_ref, back_ref, hidden_ref, scaled_ref, gate_ref, up_ref, both
):
    width = grad_ref.shape[1]
    half = weight_ref.shape[1] // 2

    @pl.when((pl.program_id(0) == 0) & (pl.program_id(1) == 0))
    def _():
        both[...] = jnp.zeros_like(both)

    acts = jnp.dot(rows_ref[...], weight_ref[...], preferred_element_type=jnp.float32)
    gate_act, up_act = acts[:, :width], acts[:, half : half + width]
    sigma = 1.0 / (1.0 + jnp.exp(-gate_act))
    silu = gate_act * sigma
    hidden = (silu * up_act).astype(jnp.bfloat16)
    hidden_ref[...] = hidden
    scaled_ref[...] = (hidden.astype(jnp.float32) * slot_ref[...]).astype(jnp.bfloat16)
    grad = grad_ref[...] * slot_ref[...]
    gate_grad = (grad * up_act * sigma * (1.0 + gate_act * (1.0 - sigma))).astype(jnp.bfloat16)
    up_grad = (grad * silu).astype(jnp.bfloat16)
    gate_ref[...] = gate_grad
    up_ref[...] = up_grad
    both[:, :width] = gate_grad
    both[:, half : half + width] = up_grad
    back_ref[...] = lax.dot_general(
        both[...], weight_ref[...], (((1,), (1,)), ((), ())), preferred_element_type=jnp.float32
    ).astype(jnp.bfloat16)


def expert_pass(rows, grad_hidden, weights, slot_weight):
    experts, slots, width = rows.shape
    hidden = grad_hidden.shape[2]
    share = slots // 2
    row_spec = pl.BlockSpec((None, share, width), lambda e, i: (e, i, 0))
    hidden_spec = pl.BlockSpec((None, share, hidden), lambda e, i: (e, i, 0))
    hidden_shape = jax.ShapeDtypeStruct((experts, slots, hidden), jnp.bfloat16)
    return pl.pallas_call(
        expert_kernel,
        grid=(experts, 2),
        in_specs=[
            row_spec,
            hidden_spec,
            pl.BlockSpec((None,) + weights.shape[1:], lambda e, i: (e, 0, 0)),
            pl.BlockSpec((None, share, 1), lambda e, i: (e, i, 0)),
        ],
        out_specs=[row_spec] + [hidden_spec] * 4,
        out_shape=[jax.ShapeDtypeStruct(rows.shape, jnp.bfloat16)] + [hidden_shape] * 4,
        scratch_shapes=[pltpu.VMEM((share, weights.shape[2]), jnp.bfloat16)],
        cost_estimate=pl.CostEstimate(
            flops=8 * experts * slots * width * hidden,
            bytes_accessed=4 * experts * (slots + hidden) * width,
            transcendentals=experts * slots * hidden,
        ),
        name="expert_pass",
    )(rows, grad_hidden, weights, slot_weight[..., None])


def side_by_side(value, ranks):
    width = value.shape[1]
    value = value.reshape(ranks, 4, -1, width).transpose(0, 2, 1, 3)
    return value.reshape(-1, 4 * width)


def stacked(value, ranks):
    width = value.shape[1] // 4
    value = value.reshape(ranks, -1, 4, width).transpose(0, 2, 1, 3)
    return value.reshape(-1, width)


def local(
    tokens,
    segments,
    expert_ids,
    route_weight,
    norm1_gain,
    q_weight,
    kva_weight,
    kv_gain,
    kvb_weight,
    out_weight,
    norm2_gain,
    shared_gate,
    shared_up,
    shared_down,
    expert_gate,
    expert_up_projection,
    expert_down,
    cotangent,
):
    length = tokens.shape[0]
    model_width = tokens.shape[1]
    groups = lax.axis_size(TP)
    rank_count = lax.axis_size(DP)
    local_experts = expert_gate.shape[0]
    experts_all = local_experts * rank_count
    choose = expert_ids.shape[1]
    capacity = groups * -(-(3 * length * choose) // (2 * experts_all * groups))
    slot_room = 16 * -(-capacity // 16)
    head_count = q_weight.shape[1] // (NOPE + ROPE)
    score_scale = (NOPE + ROPE) ** (-0.5)
    dp_index = lax.axis_index(DP)
    column = lax.axis_index(TP)
    chips = rank_count // 2
    token_share = length // groups

    def quarter(rows):
        return lax.dynamic_slice_in_dim(rows, column * token_share, token_share, 0)

    gain_widths = (norm1_gain.shape[0], kv_gain.shape[0], norm2_gain.shape[0])
    latent_rows, latent_width = kva_weight.shape
    gain_row = jnp.concatenate([norm1_gain, kv_gain, norm2_gain])
    gain_columns = -(-sum(gain_widths) // latent_rows)
    gain_row = jnp.pad(gain_row, (0, gain_columns * latent_rows - sum(gain_widths)))
    small = jnp.concatenate([kva_weight, gain_row.reshape(latent_rows, gain_columns)], axis=1)
    small = gather_dp(small)
    pieces = [small] + [shift_tensor(small, j) for j in range(1, groups)]
    pieces = tuple(pieces)
    small_all = jnp.zeros((rank_count, groups) + small.shape[1:], small.dtype)
    for j, piece in enumerate(pieces):
        small_all = lax.dynamic_update_index_in_dim(small_all, piece, (column - j) % groups, 1)
    small_all = small_all.reshape(-1, latent_width + gain_columns)
    latent_full = small_all[:, :latent_width]
    gains_all = small_all[:, latent_width:].reshape(rank_count * groups, -1).astype(jnp.float32)
    attention_norm_scale = gains_all[:, : gain_widths[0]].reshape(-1)
    latent_norm_scale = gains_all[:, gain_widths[0] : gain_widths[0] + gain_widths[1]].reshape(-1)
    feedforward_norm_scale = gains_all[:, gain_widths[0] + gain_widths[1] : sum(gain_widths)].reshape(-1)

    expand_full = gather_dp(kvb_weight, pieces).reshape(-1, kvb_weight.shape[1])
    query_full = gather_dp(q_weight, pieces).reshape(-1, q_weight.shape[1])
    output_rows = gather_dp(after(out_weight, small_all))
    output_full = output_rows.transpose(1, 0, 2).reshape(out_weight.shape[0], -1)

    routing = jnp.concatenate([expert_ids.astype(jnp.float32).T, route_weight.T], axis=0)
    routing_all = gather_dp(routing)
    ids_all, weights_all = routing_all[:, :choose].astype(jnp.int32), routing_all[:, choose:]
    grad_all = lax.all_gather(
        after(quarter(cotangent), small), (DP, TP), axis=0, tiled=True
    )
    residual_stream = tokens.astype(jnp.float32)
    inv_one = norm_scale(residual_stream)
    hat_one = residual_stream * inv_one
    normed_one = (hat_one * attention_norm_scale).astype(jnp.bfloat16)
    segment_row = segments[0]
    cosine, sine_part = angles(segment_row)
    queries = jnp.dot(normed_one, query_full, preferred_element_type=jnp.float32).reshape(
        length, head_count, NOPE + ROPE
    )
    q_rot = jnp.concatenate(
        [
            queries[..., :NOPE],
            rotate(queries[..., NOPE:], cosine[:, None, :], sine_part[:, None, :]),
        ],
        axis=-1,
    ).astype(jnp.bfloat16)
    compressed = jnp.dot(normed_one, latent_full, preferred_element_type=jnp.float32)
    latent_raw = compressed[:, :LATENT]
    inv_kv = norm_scale(latent_raw)
    hat_kv = latent_raw * inv_kv
    latent_low = (hat_kv * latent_norm_scale).astype(jnp.bfloat16)
    key_rot = rotate(compressed[:, LATENT:], cosine, sine_part).astype(jnp.bfloat16)
    keyval = (
        jnp.dot(latent_low, expand_full, preferred_element_type=jnp.float32)
        .astype(jnp.bfloat16)
        .reshape(length, head_count, NOPE + VDIM)
    )
    key_nope = keyval[..., :NOPE]
    values = keyval[..., NOPE:]
    positions = jnp.arange(length, dtype=jnp.int32)
    allowed = (segment_row[:, None] == segment_row[None, :]) & (
        positions[None, :] <= positions[:, None]
    )

    def raw_scores():
        dots = jnp.einsum(
            "thd,shd->hts", q_rot[..., :NOPE], key_nope, preferred_element_type=jnp.float32
        )
        dots = dots + jnp.einsum(
            "thr,sr->hts", q_rot[..., NOPE:], key_rot, preferred_element_type=jnp.float32
        )
        return jnp.where(allowed[None], dots * score_scale, -1000000000.0)

    scores = raw_scores()
    row_peak = jnp.max(scores, axis=-1, keepdims=True)
    log_total = jnp.log(jnp.sum(jnp.exp(scores - row_peak), axis=-1, keepdims=True)) + row_peak
    attn_probs = jnp.exp(scores - log_total)
    mixed_heads = (
        jnp.einsum(
            "hts,shv->thv",
            attn_probs.astype(jnp.bfloat16),
            values,
            preferred_element_type=jnp.float32,
        )
        .astype(jnp.bfloat16)
        .reshape(length, head_count * VDIM)
    )
    attn_out = scatter_tensor(
        jnp.dot(mixed_heads, output_full, preferred_element_type=jnp.float32).astype(jnp.bfloat16)
    )
    middle = quarter(tokens).astype(jnp.float32) + after(attn_out, grad_all)
    inv_two = norm_scale(middle)
    hat_two = middle * inv_two
    normed_two = (hat_two * feedforward_norm_scale).astype(jnp.bfloat16)
    rows_all = lax.all_gather(normed_two, (DP, TP), axis=0, tiled=True)
    feedforward_normed_input = lax.dynamic_slice_in_dim(rows_all, dp_index * length, length, 0)

    gate_lift_full = lax.all_gather(
        jnp.concatenate([shared_gate, shared_up], axis=1), DP, axis=0, tiled=True
    )
    lower_full = lax.all_gather(shared_down, DP, axis=1, tiled=True)

    slot_token, slot_weight = slot_tables(
        ids_all, weights_all, dp_index * local_experts, local_experts, slot_room
    )
    inner = groups // 2
    share = slot_token // token_share
    step = (share // inner - column // inner) % 2 * inner + (share - column) % inner
    outer_steps = jnp.arange(groups, dtype=jnp.int32) // inner
    inner_steps = jnp.arange(groups, dtype=jnp.int32) % inner
    step_starts = (column // inner + outer_steps) % 2 * inner + (column + inner_steps) % inner
    near_token = jnp.where(slot_token < 0, -1, step * token_share + slot_token % token_share)
    slot_weight = slot_weight.transpose(1, 0, 2).reshape(local_experts, -1)
    chip_steps = (dp_index // 2 + jnp.arange(chips, dtype=jnp.int32)) % chips
    own_order = 2 * chip_steps + dp_index % 2
    other_order = 2 * chip_steps + 1 - dp_index % 2
    expert_width = expert_gate.shape[2]
    lane_pad = ((0, 0), (0, 0), (0, -expert_width % 128))
    gate_up = jnp.concatenate(
        [jnp.pad(expert_gate, lane_pad), jnp.pad(expert_up_projection, lane_pad)], axis=2
    )
    grad_arrived = fetch_rows(slot_token, grad_all.reshape(rank_count, length, model_width))
    hidden_state_gradient = jnp.einsum(
        "erd,efd->erf", grad_arrived, expert_down, preferred_element_type=jnp.float32
    )
    received_rows = fetch_rows(slot_token, rows_all.reshape(rank_count, length, model_width))
    grad_inputs, expert_hidden, weighted_hidden, expert_gate_gradient, expert_up_gradient = (
        expert_pass(received_rows, hidden_state_gradient, gate_up, slot_weight)
    )

    def cut_back(rows, extra=None):
        other = return_rows(other_order, step_starts, near_token, rows, length)
        arrived = [[swap_cores(piece) for piece in half] for half in other]
        held = return_rows(
            own_order, step_starts, near_token, rows, length, extra, arrived
        )
        return held, other

    grad_cut, grad_other = cut_back(grad_inputs)
    expert_out = jnp.einsum(
        "erf,efd->erd", after(expert_hidden, grad_other[0][0]), expert_down,
        preferred_element_type=jnp.float32,
    )
    expert_out = (expert_out * slot_weight[..., None]).astype(jnp.bfloat16)
    grad_expert_down = jnp.einsum(
        "erf,erd->efd", weighted_hidden, grad_arrived, preferred_element_type=jnp.float32
    )
    grad_expert_gate = jnp.einsum(
        "erd,erf->edf", received_rows, expert_gate_gradient, preferred_element_type=jnp.float32
    )
    grad_expert_up = jnp.einsum(
        "erd,erf->edf", received_rows, expert_up_gradient, preferred_element_type=jnp.float32
    )

    hidden_width = shared_gate.shape[1]
    gate_lift_act = jnp.dot(
        feedforward_normed_input, gate_lift_full, preferred_element_type=jnp.float32
    )
    shared_gate_act, shared_up_act = gate_lift_act[:, :hidden_width], gate_lift_act[:, hidden_width:]
    shared_hidden = (jax.nn.silu(shared_gate_act) * shared_up_act).astype(jnp.bfloat16)
    shared_out = jnp.dot(shared_hidden, lower_full, preferred_element_type=jnp.float32)
    shared_out = shared_out.astype(jnp.bfloat16)
    out_cut, out_other = cut_back(expert_out, shared_out)
    block_out = scatter_all(out_cut)
    output_share = (middle + block_out).astype(jnp.bfloat16)
    output = gather_tensor(output_share)
    grad_out = quarter(cotangent).astype(jnp.float32)
    grad_shared_hidden = dot_last(cotangent, lower_full)
    grad_sgate, grad_sup = swish_derivative(grad_shared_hidden, shared_gate_act, shared_up_act)
    grad_gate_lift = jnp.concatenate(
        [grad_sgate.astype(jnp.bfloat16), grad_sup.astype(jnp.bfloat16)], axis=1
    )
    grad_lower = dot_first(shared_hidden, cotangent).astype(jnp.bfloat16)
    grad_gate_lift_full = dot_first(feedforward_normed_input, grad_gate_lift).astype(jnp.bfloat16)
    shared_grad = dot_last(grad_gate_lift, gate_lift_full).astype(jnp.bfloat16)
    shared_grad_share = scatter_tensor(shared_grad)
    routed_grad = scatter_all(
        grad_cut,
        hold_first=(out_other[0][0], shared_grad, grad_gate_lift_full),
        hold_second=(out_cut[0][0], grad_lower),
        hold_last=(grad_expert_down, grad_expert_gate, grad_expert_up),
    )
    grad_normed_two = shared_grad_share + routed_grad
    grad_gain_two = jnp.sum(grad_normed_two * hat_two, axis=0)
    grad_middle = grad_out + norm_back(grad_normed_two * feedforward_norm_scale, hat_two, inv_two)
    grad_middle_low = gather_tensor(grad_middle.astype(jnp.bfloat16))
    grad_output_full = dot_first(mixed_heads, grad_middle_low)
    grad_mixed = dot_last(grad_middle_low, output_full)
    grad_mixed = (
        grad_mixed.astype(jnp.bfloat16)
        .reshape(length, head_count, VDIM)
    )
    scores = raw_scores()
    attn_probs = jnp.exp(scores - log_total)
    grad_probs = jnp.einsum("thv,shv->hts", grad_mixed, values, preferred_element_type=jnp.float32)
    grad_values = jnp.einsum(
        "hts,thv->shv",
        attn_probs.astype(jnp.bfloat16),
        grad_mixed,
        preferred_element_type=jnp.float32,
    )
    row_delta = jnp.sum(attn_probs * grad_probs, axis=-1, keepdims=True)
    grad_scores = (attn_probs * (grad_probs - row_delta)).astype(jnp.bfloat16)
    grad_q_nope = (
        jnp.einsum("hts,shd->thd", grad_scores, key_nope, preferred_element_type=jnp.float32)
        * score_scale
    )
    grad_q_rope = (
        jnp.einsum("hts,sr->thr", grad_scores, key_rot, preferred_element_type=jnp.float32)
        * score_scale
    )
    grad_k_nope = (
        jnp.einsum(
            "hts,thd->shd", grad_scores, q_rot[..., :NOPE], preferred_element_type=jnp.float32
        )
        * score_scale
    )
    grad_k_rope = jnp.einsum(
        "hts,thr->sr", grad_scores, q_rot[..., NOPE:], preferred_element_type=jnp.float32
    )
    grad_k_rope = grad_k_rope * score_scale
    grad_queries = jnp.concatenate(
        [grad_q_nope, rotate(grad_q_rope, cosine[:, None, :], -sine_part[:, None, :])], axis=-1
    )
    grad_queries = grad_queries.astype(jnp.bfloat16).reshape(length, head_count * (NOPE + ROPE))
    grad_keyval = (
        jnp.concatenate([grad_k_nope, grad_values], axis=-1)
        .astype(jnp.bfloat16)
        .reshape(length, head_count * (NOPE + VDIM))
    )
    grad_query_full = dot_first(normed_one, grad_queries)
    grad_expand_full = dot_first(latent_low, grad_keyval)
    grad_latent = dot_last(grad_keyval, expand_full)
    grad_gain_kv = jnp.sum(grad_latent * hat_kv, axis=0)
    grad_latent_raw = norm_back(grad_latent * latent_norm_scale, hat_kv, inv_kv)
    grad_compressed = jnp.concatenate(
        [grad_latent_raw, rotate(grad_k_rope, cosine, -sine_part)], axis=-1
    ).astype(jnp.bfloat16)
    grad_latent_full = dot_first(normed_one, grad_compressed).astype(jnp.bfloat16)
    grad_latent_full = grad_latent_full.reshape((rank_count, groups) + kva_weight.shape)
    latent_parts = [pick(grad_latent_full, column, 1)] + [
        shift_tensor(pick(grad_latent_full, (column + j) % groups, 1), j)
        for j in range(1, groups)
    ]
    grad_normed_one = dot_last(grad_queries, query_full)
    grad_normed_one = grad_normed_one + dot_last(grad_compressed, latent_full)
    grad_gate_lift_share = lax.psum_scatter(
        grad_gate_lift_full, DP, scatter_dimension=0, tiled=True
    ).astype(jnp.float32)
    grad_shared_gate = grad_gate_lift_share[:, :hidden_width]
    grad_shared_up = grad_gate_lift_share[:, hidden_width:]
    grad_shared_down = lax.psum_scatter(
        grad_lower, DP, scatter_dimension=1, tiled=True
    ).astype(jnp.float32)
    grad_out_weight = lax.psum_scatter(
        grad_output_full.astype(jnp.bfloat16), DP, scatter_dimension=1, tiled=True
    ).astype(jnp.float32)
    grad_normed_one = grad_normed_one.astype(jnp.bfloat16)
    grad_latent_part = total([after(latent_parts[0], grad_query_full)] + latent_parts[1:])
    grad_normed_one = scatter_tensor(grad_normed_one)
    hat_one_share = quarter(hat_one)
    grad_gain_one = jnp.sum(grad_normed_one * hat_one_share, axis=0)
    grad_tokens = grad_middle + norm_back(
        grad_normed_one * attention_norm_scale, hat_one_share, quarter(inv_one)
    )
    grad_tokens = gather_tensor(grad_tokens.astype(jnp.bfloat16)).astype(jnp.float32)

    query_width, expand_width = 4 * q_weight.shape[1], kvb_weight.shape[1]
    packed_rows = grad_expand_full.shape[0]
    packed_grad = jnp.concatenate(
        [
            side_by_side(grad_query_full.astype(jnp.bfloat16), rank_count),
            grad_expand_full.astype(jnp.bfloat16),
            grad_latent_part.astype(jnp.bfloat16).reshape(packed_rows, -1),
        ],
        axis=1,
    )
    packed_share = lax.psum_scatter(packed_grad, DP, scatter_dimension=0, tiled=True)
    grad_q_weight = stacked(packed_share[:, :query_width], 1).astype(jnp.float32)
    grad_kvb_weight = packed_share[:, query_width : query_width + expand_width].astype(jnp.float32)
    grad_kva_weight = packed_share[:, query_width + expand_width :].astype(jnp.float32)
    grad_kva_weight = grad_kva_weight.reshape(kva_weight.shape)
    gain_grads = jnp.concatenate(
        [
            grad.reshape(rank_count, groups, -1)
            for grad in (grad_gain_one, grad_gain_kv, grad_gain_two)
        ],
        axis=2,
    )
    gain_grads = scatter_small(
        gain_grads, (grad_shared_gate, grad_shared_up, grad_shared_down, grad_out_weight)
    )
    grad_norm1_gain = gain_grads[: gain_widths[0]]
    grad_kv_gain = gain_grads[gain_widths[0] : gain_widths[0] + gain_widths[1]]
    grad_norm2_gain = gain_grads[gain_widths[0] + gain_widths[1] :]
    return (
        output,
        grad_tokens,
        grad_norm1_gain,
        grad_q_weight,
        grad_kva_weight,
        grad_kv_gain,
        grad_kvb_weight,
        grad_out_weight,
        grad_norm2_gain,
        grad_shared_gate,
        grad_shared_up,
        grad_shared_down,
        grad_expert_gate,
        grad_expert_up,
        grad_expert_down,
    )


def solution(mesh):
    in_specs = (
        P(DP, None),
        P(DP, None),
        P(DP, None),
        P(DP, None),
        P((DP, TP)),
        P(DP, TP),
        P((DP, TP), None),
        P((DP, TP)),
        P(DP, TP),
        P(TP, DP),
        P((DP, TP)),
        P(DP, TP),
        P(DP, TP),
        P(TP, DP),
        P(DP, None, TP),
        P(DP, None, TP),
        P(DP, TP, None),
        P(DP, None),
    )
    out_specs = (
        P(DP, None),
        P(DP, None),
        P((DP, TP)),
        P(DP, TP),
        P((DP, TP), None),
        P((DP, TP)),
        P(DP, TP),
        P(TP, DP),
        P((DP, TP)),
        P(DP, TP),
        P(DP, TP),
        P(TP, DP),
        P(DP, None, TP),
        P(DP, None, TP),
        P(DP, TP, None),
    )

    return jax.shard_map(local, mesh=mesh, in_specs=in_specs, out_specs=out_specs, check_vma=False)
```
